128 devices in a mesh: ka: 32 (over z, y, core), col: 4 (over x).
Axes of the slice: x: 4, y: 4, z: 4, core: 2. Of those that a mesh axis runs over, the one named last changes fastest.
Arguments:
- hamiltonian: bfloat16 [1024, 2, 9216], P(('ka', 'col')), may hold values from -0.1875 to 0.1875
- eigvecs: bfloat16 [2048, 2, 96, 96], P('ka'), may hold values from -0.625 to 0.625
- spin: bfloat16 [2, 96, 96], replicated, may hold values from -0.059814453 to 0.059814453
- k_indices: int32 [2048, 3], P('ka'), may hold values from 0 to 63
- r_vectors: int32 [1024, 3], replicated, may hold values from -5 to 5, as said below
- degeneracy: int32 [1024], replicated, may hold values from 1 to 4
- fermi_level: float32 [1], replicated, may hold values from -0.5 to 0.5
Outputs:
- band_curvature: float32 [9, 96, 2048], P(None, None, ('ka', 'col'))
- conductivity: float32 [9, 96], replicated
The draws below stay inside these ranges and needn't reach their ends.
Inputs may be any that keep to these rules, and one draw needn't show every extreme that they name: `r_vectors`: the 1024 lattice vectors are all distinct.
All inputs are finite; a program needn't handle non-finite values.
Results may differ from the reference program's by a relative error of at most 0.0085.
The reference program's roundings to bfloat16 on the way count: a program that leaves them out, or rounds other values in their place, can miss the bound.
Values may be sent and summed in bfloat16 or wider, within the bound.
No kernel may reach another device: no remote copies, remote signals or barrier semaphores. Data moves between devices by JAX's collectives and lax.ppermute only.
A program may use at most 128 MiB of HBM per device.

```python
import math
import jax
import jax.numpy as jnp
from jax import lax

WF = 96
NR = 1024
K_DEV = 64
GRID = 64
NK = 2048


def draw_r_vectors(key, part):
    codes = jax.random.permutation(jax.random.fold_in(key, 17), jnp.arange(1331, dtype=jnp.int32))[:NR]
    first = codes // 121
    second = codes // 11 % 11
    third = codes % 11
    return (jnp.stack([first, second, third], axis=1) - 5).astype(jnp.int32)


def place_ends(entries, key, least, top_value):
    longest = entries.shape.index(max(entries.shape))
    spots = []
    for shift in (0, 1):
        where = [jax.random.randint(jax.random.fold_in(key, axis), (), 0, length) for axis, length in enumerate(entries.shape)]
        where[longest] = (where[longest] + shift) % entries.shape[longest]
        spots.append(tuple(where))
    return entries.at[spots[0]].set(least).at[spots[1]].set(top_value)


def block_levels(stream_key, extent, split, least, largest):
    def one(axis_at, parts):
        draws = jax.random.uniform(jax.random.fold_in(jax.random.fold_in(stream_key, 6), axis_at), (parts,), jnp.float32, least / len(split), largest / len(split))
        return jnp.repeat(jnp.exp(draws), extent[axis_at] // parts).reshape((-1,) + (1,) * (len(extent) - axis_at - 1))

    loudness = one(*split[0])
    for cut in split[1:]:
        loudness = loudness * one(*cut)
    return loudness


def bell_draw(rng, extent, scale, bound, cuts=(), kind=jnp.bfloat16):
    entries = scale * jax.random.normal(rng, extent, jnp.float32)
    if cuts:
        entries = entries * block_levels(rng, extent, cuts, -0.22, 0.18)
    return jnp.clip(entries, -bound, bound).astype(kind)


def setup_inputs(seed: int = 0) -> dict:
    keys = jax.random.split(jax.random.key(seed), 8)
    hamiltonian = bell_draw(keys[0], (NR, 2, WF * WF), NR ** -0.5, 0.1875, ((0, 128),))
    eigvecs = bell_draw(keys[1], (NK, 2, WF, WF), WF ** -0.5, 0.625, ((0, 32),))
    spin = bell_draw(keys[2], (2, WF, WF), 0.01, 0.059814453)
    k_indices = place_ends(jax.random.randint(keys[3], (NK, 3), 0, GRID), jax.random.fold_in(keys[3], 1), 0, GRID - 1).astype(jnp.int32)
    r_vectors = draw_r_vectors(jax.random.fold_in(keys[7], 71), 0)
    degeneracy = place_ends(jax.random.randint(keys[5], (NR,), 1, 5), jax.random.fold_in(keys[5], 1), 1, 4).astype(jnp.int32)
    fermi_level = jnp.clip(jax.random.uniform(keys[6], (1,), jnp.float32, -0.5, 0.5), -0.5, 0.5)
    return {"hamiltonian": hamiltonian, "eigvecs": eigvecs, "spin": spin, "k_indices": k_indices, "r_vectors": r_vectors, "degeneracy": degeneracy, "fermi_level": fermi_level}


two_pi = 2.0 * math.pi
broadening = 0.5
smearing = 0.1

def phase_table(kpoints, lattice, degrees):
    lattice_dot = jnp.mod(lax.optimization_barrier(jnp.sum(kpoints[:, None, :] * lattice[None, :, :], axis=-1)), GRID)
    angles = lattice_dot.astype(jnp.float32) * (two_pi / GRID)
    cosine = jnp.cos(angles)
    sine_part = jnp.sin(angles)
    inverse = 1.0 / degrees.astype(jnp.float32)
    coords = lattice.astype(jnp.float32) * inverse[:, None]
    real_part = jnp.stack([cosine * inverse, -sine_part * coords[:, 0], -sine_part * coords[:, 1], -sine_part * coords[:, 2]], axis=1)
    imag_part = jnp.stack([sine_part * inverse, cosine * coords[:, 0], cosine * coords[:, 1], cosine * coords[:, 2]], axis=1)
    top_rows = jnp.stack([real_part, -imag_part], axis=-1)
    low_rows = jnp.stack([imag_part, real_part], axis=-1)
    return jnp.stack([top_rows, low_rows], axis=2)

def rotate(operators, vectors):
    ops_re = operators[:, :, 0].astype(jnp.float32)
    ops_im = operators[:, :, 1].astype(jnp.float32)
    vec_re = vectors[:, 0].astype(jnp.float32)
    vec_im = vectors[:, 1].astype(jnp.float32)
    half_re = jnp.einsum('kcij,kjm->kcim', ops_re, vec_re) - jnp.einsum('kcij,kjm->kcim', ops_im, vec_im)
    half_im = jnp.einsum('kcij,kjm->kcim', ops_re, vec_im) + jnp.einsum('kcij,kjm->kcim', ops_im, vec_re)
    half_re = lax.optimization_barrier(half_re.astype(jnp.bfloat16)).astype(jnp.float32)
    half_im = lax.optimization_barrier(half_im.astype(jnp.bfloat16)).astype(jnp.float32)
    full_re = jnp.einsum('kjn,kcjm->kcnm', vec_re, half_re) + jnp.einsum('kjn,kcjm->kcnm', vec_im, half_im)
    full_im = jnp.einsum('kjn,kcjm->kcnm', vec_re, half_im) - jnp.einsum('kjn,kcjm->kcnm', vec_im, half_re)
    sym_re = (full_re + jnp.swapaxes(full_re, -1, -2)) * 0.5
    sym_im = (full_im - jnp.swapaxes(full_im, -1, -2)) * 0.5
    return jnp.stack([sym_re, sym_im], axis=2).astype(jnp.bfloat16)

def kubo(bloch_ops, spin_bloch, fermi_level):
    energy = jnp.diagonal(bloch_ops[:, 0, 0].astype(jnp.float32), axis1=-2, axis2=-1)
    velo_re = bloch_ops[:, 1:, 0].astype(jnp.float32)
    velo_im = bloch_ops[:, 1:, 1].astype(jnp.float32)
    spin_re = spin_bloch[:, 0].astype(jnp.float32)
    spin_im = spin_bloch[:, 1].astype(jnp.float32)
    prod_re = jnp.einsum('kij,kajm->kaim', spin_re, velo_re) - jnp.einsum('kij,kajm->kaim', spin_im, velo_im)
    prod_im = jnp.einsum('kij,kajm->kaim', spin_re, velo_im) + jnp.einsum('kij,kajm->kaim', spin_im, velo_re)
    cur_re = (prod_re + jnp.swapaxes(prod_re, -1, -2)) * 0.5
    cur_im = (prod_im - jnp.swapaxes(prod_im, -1, -2)) * 0.5
    energy_gap = energy[:, :, None] - energy[:, None, :]
    weight = 1.0 / (energy_gap * energy_gap + broadening * broadening)
    curvature = -2.0 * (jnp.einsum('kanm,kbmn,knm->kabn', cur_re, velo_im, weight) + jnp.einsum('kanm,kbmn,knm->kabn', cur_im, velo_re, weight))
    occupation = 1.0 / (1.0 + jnp.exp((energy - fermi_level[0]) / smearing))
    weighted = jnp.einsum('kn,kabn->abn', occupation, curvature)
    return (curvature, weighted)

def reference(hamiltonian, eigvecs, spin, k_indices, r_vectors, degeneracy, fermi_level):
    block_count = NK // K_DEV
    hopping = hamiltonian.reshape(NR * 2, WF * WF)
    spin_wide = spin.astype(jnp.float32)
    spin_sym = jnp.stack([(spin_wide[0] + spin_wide[0].T) * 0.5, (spin_wide[1] - spin_wide[1].T) * 0.5]).astype(jnp.bfloat16)

    def one_block(block_index):
        kpoints = lax.dynamic_slice_in_dim(k_indices, block_index * K_DEV, K_DEV, 0)
        vectors = lax.dynamic_slice_in_dim(eigvecs, block_index * K_DEV, K_DEV, 0)
        phases = phase_table(kpoints, r_vectors, degeneracy).reshape(K_DEV * 8, NR * 2).astype(jnp.bfloat16)
        summed = jnp.dot(phases, hopping, preferred_element_type=jnp.float32)
        interpolated = summed.reshape(K_DEV, 4, 2, WF, WF).astype(jnp.bfloat16)
        bloch_ops = rotate(interpolated, vectors)
        spin_ops = jnp.broadcast_to(spin_sym[None, None], (K_DEV, 1, 2, WF, WF))
        spin_bloch = rotate(spin_ops, vectors)[:, 0]
        return kubo(bloch_ops, spin_bloch, fermi_level)
    curvature, weighted = lax.map(one_block, jnp.arange(block_count, dtype=jnp.int32))
    curvature = curvature.reshape(NK, 3, 3, WF)
    band_curvature = jnp.transpose(curvature, (1, 2, 3, 0)).reshape(9, WF, NK)
    conductivity = (lax.optimization_barrier(jnp.sum(weighted, axis=0)) / math.sqrt(NK)).reshape(9, WF)
    return (band_curvature, conductivity)
```

```python
import math

import jax
import jax.numpy as jnp
from jax import lax
from jax.experimental import pallas as pl
from jax.experimental.pallas import tpu as pltpu
from jax.sharding import Mesh, PartitionSpec as P

WF = 96
GRID = 64
NR = 1024
GROUP = 32
ROWS = 3
PIECE = ROWS * 2 * WF
WIDE = 640
KEPT = 4 * PIECE
QUARTER = 16
STEP_K = 128
PER_STEP = 2

two_pi = 2.0 * math.pi
broadening = 0.5
smearing = 0.1

ALL = ("z", "y", "core", "x")
PLANE = ("y", "core", "x")

f32 = jnp.float32
bf16 = jnp.bfloat16


def half_turn(count):
    y = count * (math.pi / GRID)
    q = y * y
    s = 1.0 - q * (1.0 / 110.0)
    s = 1.0 - q * (1.0 / 72.0) * s
    s = 1.0 - q * (1.0 / 42.0) * s
    s = 1.0 - q * (1.0 / 20.0) * s
    s = 1.0 - q * (1.0 / 6.0) * s
    s = y * s
    c = 1.0 - q * (1.0 / 132.0)
    c = 1.0 - q * (1.0 / 90.0) * c
    c = 1.0 - q * (1.0 / 56.0) * c
    c = 1.0 - q * (1.0 / 30.0) * c
    c = 1.0 - q * (1.0 / 12.0) * c
    c = 1.0 - q * (1.0 / 2.0) * c
    return 1.0 - 2.0 * s * s, 2.0 * s * c


def interpolate_kernel(k_ref, lat_ref, hop_ref, out_ref, w_ref, p_ref):
    @pl.when(pl.program_id(0) == 0)
    def _():
        lane = lax.broadcasted_iota(jnp.int32, (NR, 128), 1)
        tiles = [hop_ref[:, 128 * t : 128 * (t + 1)].astype(f32) for t in range(5)]
        tiles[4] = jnp.where(lane < 64, tiles[4], 0.0)
        ups = [pltpu.roll(t, 96, 1) for t in tiles]
        downs = [pltpu.roll(t, 32, 1) for t in tiles]
        for t in range(5):
            w_ref[0:NR, 128 * t : 128 * (t + 1)] = tiles[t].astype(bf16)
            before = ups[(t - 1) % 5]
            after = downs[(t + 1) % 5]
            up = jnp.where(lane < 96, before, ups[t])
            down = jnp.where(lane < 32, downs[t], after)
            place = (lane + 128 * t) % (2 * WF)
            turned = jnp.where(place < WF, -down, up)
            if t == 4:
                turned = jnp.where(lane < 64, turned, 0.0)
            w_ref[NR : 2 * NR, 128 * t : 128 * (t + 1)] = turned.astype(bf16)

    k = k_ref[...]
    r0 = lat_ref[0:1, :]
    r1 = lat_ref[1:2, :]
    r2 = lat_ref[2:3, :]
    inverse = 1.0 / lat_ref[3:4, :]
    dots = k[:, 0:1] * r0 + k[:, 1:2] * r1 + k[:, 2:3] * r2
    count = dots - 64.0 * jnp.floor(dots * (1.0 / 64.0) + 0.5)
    cosine, sine = half_turn(count)
    coords = [r0 * inverse, r1 * inverse, r2 * inverse]
    for c in range(4):
        rows = slice(c * STEP_K, (c + 1) * STEP_K)
        if c == 0:
            re, im = cosine * inverse, sine * inverse
        else:
            re, im = -sine * coords[c - 1], cosine * coords[c - 1]
        p_ref[rows, 0:NR] = re.astype(bf16)
        p_ref[rows, NR : 2 * NR] = im.astype(bf16)
    summed = jnp.dot(p_ref[...], w_ref[...], preferred_element_type=f32)
    lane = lax.broadcasted_iota(jnp.int32, (STEP_K, 128), 1)
    for pair in range(2):
        even = summed[2 * pair * STEP_K : (2 * pair + 1) * STEP_K]
        odd = summed[(2 * pair + 1) * STEP_K : (2 * pair + 2) * STEP_K]
        shifted = [pltpu.roll(odd[:, 128 * t : 128 * (t + 1)], 64, 1) for t in range(5)]
        for t in range(9):
            if t < 4:
                tile = even[:, 128 * t : 128 * (t + 1)]
            elif t == 4:
                tile = jnp.where(lane < 64, even[:, 512:640], shifted[0])
            else:
                tile = jnp.where(lane < 64, shifted[t - 5], shifted[t - 4])
            at = pair * 2 * PIECE + 128 * t
            out_ref[:, :, at : at + 128] = tile.reshape(STEP_K // QUARTER, QUARTER, 128).astype(bf16)


def interpolate(k_rows, lattice, hopping):
    per = STEP_K // QUARTER
    return pl.pallas_call(
        interpolate_kernel,
        grid=(GROUP * QUARTER // STEP_K,),
        in_specs=[
            pl.BlockSpec((STEP_K, 8), lambda i: (i, 0)),
            pl.BlockSpec((8, NR), lambda i: (0, 0)),
            pl.BlockSpec((NR, WIDE), lambda i: (0, 0)),
        ],
        out_specs=pl.BlockSpec((per, QUARTER, KEPT), lambda i: (i, 0, 0)),
        out_shape=jax.ShapeDtypeStruct((GROUP, QUARTER, KEPT), bf16),
        scratch_shapes=[
            pltpu.VMEM((2 * NR, WIDE), bf16),
            pltpu.VMEM((4 * STEP_K, 2 * NR), bf16),
        ],
        compiler_params=pltpu.CompilerParams(
            dimension_semantics=("arbitrary",), vmem_limit_bytes=40 << 20
        ),
        name="interpolate",
    )(k_rows, lattice, hopping)


def flip(x):
    return jnp.transpose(x, (1, 0))


def bands_kernel(
    vec_ref, got_ref, spin_ref, fermi_ref, curve_ref, total_ref,
    wide_ref, we_ref, wo_ref, sp_ref, ut_ref, rh_ref, keep_ref, sum_ref,
):
    step = pl.program_id(0)

    @pl.when(step == 0)
    def _():
        for t in range(KEPT // 128):
            tile = got_ref[:, :, 128 * t : 128 * (t + 1)].astype(f32)
            wide_ref[t] = tile.reshape(GROUP * QUARTER, 128)
        we_ref[...] = jnp.zeros_like(we_ref)
        wo_ref[...] = jnp.zeros_like(wo_ref)
        ut_ref[...] = jnp.zeros_like(ut_ref)
        rh_ref[...] = jnp.zeros_like(rh_ref)
        sum_ref[...] = jnp.zeros_like(sum_ref)
        keep_ref[...] = jnp.zeros_like(keep_ref)
        sp_ref[...] = jnp.zeros_like(sp_ref)
        spin_re = spin_ref[0].astype(f32)
        spin_im = spin_ref[1].astype(f32)
        sym_re = (spin_re + flip(spin_re)) * 0.5
        sym_im = (spin_im - flip(spin_im)) * 0.5
        sp_ref[:, 0:WF] = sym_re.astype(bf16)
        sp_ref[:, WF : 2 * WF] = sym_im.astype(bf16)

    lane = lax.broadcasted_iota(jnp.int32, (WF, 128), 1)
    row = lax.broadcasted_iota(jnp.int32, (WF, 128), 0)
    eye = lane == row
    fermi = fermi_ref[0, 0]

    for q in range(PER_STEP):
        k = step * PER_STEP + q
        u_re = vec_ref[q, 0]
        u_im = vec_ref[q, 1]
        for ref, at in ((we_ref, 0), (wo_ref, 64)):
            ref[q, at : at + WF, 0:WF] = u_re
            ref[q, at : at + WF, 128 : 128 + WF] = u_im
            ref[q, at + WF : at + 2 * WF, 0:WF] = -u_im
            ref[q, at + WF : at + 2 * WF, 128 : 128 + WF] = u_re
        ut_ref[q, :, 0:WF] = flip(u_re.astype(f32)).astype(bf16)
        ut_ref[q, :, 128 : 128 + WF] = flip(u_im.astype(f32)).astype(bf16)

        def window(c, r):
            at = c * PIECE + r * 2 * WF
            first = at // 128
            parts = [
                wide_ref[first + j, pl.ds(k, GROUP, stride=QUARTER), :].astype(bf16)
                for j in range(2)
            ]
            return jnp.concatenate(parts, axis=1), at % 128 != 0

        groups = {False: [], True: []}
        where = {}
        for c in range(4):
            for r in range(ROWS):
                value, odd = window(c, r)
                where[c, r] = (odd, 32 * len(groups[odd]))
                groups[odd].append(value)
        even_rows = jnp.concatenate(groups[False] + [sp_ref[...]], axis=0)
        odd_rows = jnp.concatenate(groups[True], axis=0)
        halves = {
            False: jnp.dot(even_rows, we_ref[q], preferred_element_type=f32).astype(bf16),
            True: jnp.dot(odd_rows, wo_ref[q], preferred_element_type=f32).astype(bf16),
        }
        blochs = []
        for c in range(5):
            if c < 4:
                parts = []
                for r in range(ROWS):
                    odd, at = where[c, r]
                    parts.append(halves[odd][at : at + 32])
                half = jnp.concatenate(parts, axis=0)
            else:
                half = halves[False][192:288]
            h_re = half[:, 0:128]
            h_im = half[:, 128:256]
            rh_ref[q, c, 0:WF, 0:128] = h_re
            rh_ref[q, c, 0:WF, 128:256] = h_im
            rh_ref[q, c, 128 : 128 + WF, 0:128] = h_im
            rh_ref[q, c, 128 : 128 + WF, 128:256] = -h_re
            full = jnp.dot(ut_ref[q], rh_ref[q, c], preferred_element_type=f32)
            f_re = full[:, 0:128]
            f_im = full[:, 128:256]
            pad = jnp.zeros((32, 128), f32)
            t_re = flip(jnp.concatenate([f_re, pad], axis=0))[0:WF]
            t_im = flip(jnp.concatenate([f_im, pad], axis=0))[0:WF]
            b_re = ((f_re + t_re) * 0.5).astype(bf16)
            b_im = ((f_im - t_im) * 0.5).astype(bf16)
            blochs.append((b_re, b_im))
        diag = jnp.where(eye, blochs[0][0].astype(f32), 0.0)
        e_row = jnp.sum(diag, axis=0, keepdims=True)
        e_col = jnp.sum(diag, axis=1, keepdims=True)
        gap = e_col - e_row
        weight = -2.0 / (gap * gap + broadening * broadening)
        occupation = 1.0 / (1.0 + jnp.exp((e_row - fermi) / smearing))
        s_re, s_im = blochs[4]
        lhs = jnp.concatenate([s_re, s_im], axis=1)
        wides = [(b[0].astype(f32), b[1].astype(f32)) for b in blochs[1:4]]
        for a in range(3):
            v_re, v_im = blochs[1 + a]
            zero = jnp.zeros((32, 256), bf16)
            rhs = jnp.concatenate(
                [
                    jnp.concatenate([v_re, v_im], axis=1),
                    zero,
                    jnp.concatenate([-v_im, v_re], axis=1),
                    zero,
                ],
                axis=0,
            )
            prod = jnp.dot(lhs, rhs, preferred_element_type=f32)
            p_re = prod[:, 0:128]
            p_im = prod[:, 128:256]
            pad = jnp.zeros((32, 128), f32)
            t_re = flip(jnp.concatenate([p_re, pad], axis=0))[0:WF]
            t_im = flip(jnp.concatenate([p_im, pad], axis=0))[0:WF]
            c_re = (p_re + t_re) * 0.5 * weight
            c_im = (p_im - t_im) * 0.5 * weight
            for b in range(3):
                w_re, w_im = wides[b]
                curve = jnp.sum(c_re * w_im - c_im * w_re, axis=0, keepdims=True)
                keep_ref[3 * a + b, pl.ds(k, 1), :] = curve
                sum_ref[3 * a + b : 3 * a + b + 1, :] += occupation * curve

    @pl.when(step == pl.num_programs(0) - 1)
    def _():
        for ab in range(9):
            rows = jnp.concatenate([keep_ref[ab], jnp.zeros((112, 128), f32)], axis=0)
            curve_ref[ab] = flip(rows)[0:WF, 0:QUARTER]
        sums = sum_ref[0:8, :]
        last = jnp.broadcast_to(sum_ref[8:9, :], (8, 128))
        lane8 = lax.broadcasted_iota(jnp.int32, (8, 128), 1)
        row8 = lax.broadcasted_iota(jnp.int32, (8, 128), 0)
        extra = jnp.zeros((8, 128), f32)
        for t in range(3):
            extra = jnp.where(row8 == t, pltpu.roll(last, 96 - 32 * t, 1), extra)
        packed = jnp.where(lane8 < WF, sums, extra)
        total_ref[...] = packed


def bands(column, vectors, got, spin, fermi):
    per = QUARTER // PER_STEP
    grid_spec = pltpu.PrefetchScalarGridSpec(
        num_scalar_prefetch=1,
        grid=(per,),
        in_specs=[
            pl.BlockSpec((PER_STEP, 2, WF, WF), lambda i, c: (c[0] * per + i, 0, 0, 0)),
            pl.BlockSpec((GROUP, QUARTER, KEPT), lambda i, c: (0, 0, 0)),
            pl.BlockSpec((2, WF, WF), lambda i, c: (0, 0, 0)),
            pl.BlockSpec(memory_space=pltpu.SMEM),
        ],
        out_specs=[
            pl.BlockSpec((9, WF, QUARTER), lambda i, c: (0, 0, 0)),
            pl.BlockSpec((8, 128), lambda i, c: (0, 0)),
        ],
        scratch_shapes=[
            pltpu.VMEM((KEPT // 128, GROUP * QUARTER, 128), f32),
            pltpu.VMEM((PER_STEP, 256, 256), bf16),
            pltpu.VMEM((PER_STEP, 256, 256), bf16),
            pltpu.VMEM((WF, 256), bf16),
            pltpu.VMEM((PER_STEP, WF, 256), bf16),
            pltpu.VMEM((PER_STEP, 5, 256, 256), bf16),
            pltpu.VMEM((9, QUARTER, 128), f32),
            pltpu.VMEM((16, 128), f32),
        ],
    )

    def kernel(column_ref, *refs):
        bands_kernel(*refs)

    return pl.pallas_call(
        kernel,
        grid_spec=grid_spec,
        out_shape=[
            jax.ShapeDtypeStruct((9, WF, QUARTER), f32),
            jax.ShapeDtypeStruct((8, 128), f32),
        ],
        compiler_params=pltpu.CompilerParams(
            dimension_semantics=("arbitrary",), vmem_limit_bytes=40 << 20
        ),
        name="bands",
    )(column, vectors, got, spin, fermi)


def exchange(value, axes):
    return lax.all_to_all(value, axes, split_axis=0, concat_axis=0, tiled=True)


def on_device(hamiltonian, eigvecs, spin, k_indices, r_vectors, degeneracy, fermi_level):
    own = hamiltonian.shape[0]
    pieces = hamiltonian.reshape(own, 2, ROWS, GROUP, WF).transpose(3, 0, 2, 1, 4)
    pieces = pieces.reshape(GROUP, own, PIECE)
    points = jnp.zeros((own, WIDE - PIECE), bf16).at[0:3, :].set(k_indices.T.astype(bf16))
    points = jnp.broadcast_to(points[None], (GROUP, own, WIDE - PIECE))
    pieces = jnp.concatenate([pieces, points], axis=2)
    pieces = jnp.broadcast_to(pieces[None], (4, GROUP, own, WIDE)).reshape(4 * GROUP, own, WIDE)
    hopping = exchange(pieces, ALL)
    layer = lax.axis_index("z")
    mine = lax.dynamic_slice(hopping, (layer * GROUP, 0, 0), (GROUP, own, WIDE))
    k_rows = mine.reshape(8, 4, own, WIDE)[:, 0, :, PIECE:]
    k_rows = k_rows.transpose(0, 2, 1).reshape(8 * (WIDE - PIECE), own).astype(f32)
    lattice = jnp.concatenate(
        [r_vectors.T.astype(f32), jnp.broadcast_to(degeneracy.astype(f32)[None], (5, NR))], axis=0
    )
    entries = interpolate(k_rows, lattice, hopping.reshape(NR, WIDE))
    got = exchange(entries, PLANE)
    column = lax.axis_index("x").astype(jnp.int32).reshape(1)
    curvature, packed = bands(column, eigvecs, got, spin, fermi_level.reshape(1, 1))
    count = lax.axis_size("z") * lax.axis_size("y") * lax.axis_size("core") * lax.axis_size("x")
    copies = jnp.broadcast_to(packed[None], (count, 8, 128))
    total = jnp.sum(exchange(copies, ALL), axis=0) * (1.0 / math.sqrt(k_indices.shape[0] * 32))
    last = total[0:3, WF:].reshape(1, WF)
    totals = jnp.concatenate([total[:, :WF], last], axis=0)
    return (curvature, totals)


def solution(mesh):
    fine = Mesh(mesh.devices.reshape(4, 4, 2, 4), ALL)
    ka = ("z", "y", "core")
    in_specs = (P(ALL, None, None), P(ka, None, None, None), P(), P(ka, None), P(), P(), P())
    out_specs = (P(None, None, ALL), P())
    return jax.shard_map(
        on_device, mesh=fine, in_specs=in_specs, out_specs=out_specs, check_vma=False
    )
```

```python
import math

import jax
import jax.numpy as jnp
from jax import lax
from jax.experimental import pallas as pl
from jax.experimental.pallas import tpu as pltpu
from jax.sharding import Mesh, PartitionSpec as P

WF = 96
GRID = 64
NR = 1024
GROUP = 32
ROWS = 3
PIECE = ROWS * 2 * WF
WIDE = 640
KEPT = 4 * PIECE
QUARTER = 16
PITCH = 17
STEP_K = 128
PER_STEP = 4
SIDE_STEP = 4

broadening = 0.5
smearing = 0.1

ALL = ("z", "y", "core", "x")
PLANE = ("y", "core", "x")

f32 = jnp.float32
bf16 = jnp.bfloat16

SINE = (3.14159264, -5.16771009, 2.55007766, -0.59829216, 0.07765941)
COSINE = (0.99999995, -4.93479286, 4.05841192, -1.33188016, 0.2196968)


def whole(shape):
    return pl.BlockSpec(shape, lambda *_: (0,) * len(shape))


def horner(coefficients, q):
    value = coefficients[-1]
    for c in coefficients[-2::-1]:
        value = value * q + c
    return value


def turn(f):
    q = f * f
    s = f * horner(SINE, q)
    twice = s + s
    return 1.0 - twice * s, twice * horner(COSINE, q)


def flip(x):
    return jnp.transpose(x, (1, 0))


def flip_square(x):
    pad = jnp.zeros((32, 128), f32)
    return flip(jnp.concatenate([x, pad], axis=0))[0:WF]


def turn_hopping(hop_ref, w_ref):
    lane = lax.broadcasted_iota(jnp.int32, (NR, 128), 1)
    tiles = [hop_ref[:, 128 * t : 128 * (t + 1)].astype(f32) for t in range(5)]
    tiles[4] = jnp.where(lane < 64, tiles[4], 0.0)
    ups = [pltpu.roll(t, 96, 1) for t in tiles]
    downs = [pltpu.roll(t, 32, 1) for t in tiles]
    for t in range(5):
        w_ref[0:NR, 128 * t : 128 * (t + 1)] = tiles[t].astype(bf16)
        up = jnp.where(lane < 96, ups[(t - 1) % 5], ups[t])
        down = jnp.where(lane < 32, downs[t], downs[(t + 1) % 5])
        place = (lane + 128 * t) % (2 * WF)
        turned = jnp.where(place < WF, -down, up)
        if t == 4:
            turned = jnp.where(lane < 64, turned, 0.0)
        w_ref[NR : 2 * NR, 128 * t : 128 * (t + 1)] = turned.astype(bf16)


def phase_block(k, lat_ref, p_ref):
    r = [lat_ref[a : a + 1, :] for a in range(3)]
    inverse = 1.0 / lat_ref[3:4, :]
    turns = sum(k[:, a : a + 1] * (r[a] * (1.0 / GRID)) for a in range(3))
    cosine, sine = turn(turns - jnp.floor(turns + 0.5))
    for c in range(4):
        rows = slice(c * STEP_K, (c + 1) * STEP_K)
        if c == 0:
            re, im = cosine * inverse, sine * inverse
        else:
            coord = r[c - 1] * inverse
            re, im = sine * (-coord), cosine * coord
        p_ref[rows, 0:NR] = re.astype(bf16)
        p_ref[rows, NR : 2 * NR] = im.astype(bf16)


def interpolate_kernel(k_ref, lat_ref, hop_ref, out_ref, w_ref, *p_refs):
    steps = GROUP * QUARTER // STEP_K
    per = STEP_K // QUARTER
    lane = lax.broadcasted_iota(jnp.int32, (STEP_K, 128), 1)

    def phases(i):
        phase_block(k_ref[i * STEP_K : (i + 1) * STEP_K, :], lat_ref, p_refs[i % 2])

    phases(0)
    turn_hopping(hop_ref, w_ref)
    for i in range(steps):
        if i + 1 < steps:
            phases(i + 1)
        summed = jnp.dot(p_refs[i % 2][...], w_ref[...], preferred_element_type=f32)
        for pair in range(2):
            even = summed[2 * pair * STEP_K : (2 * pair + 1) * STEP_K]
            odd = summed[(2 * pair + 1) * STEP_K : (2 * pair + 2) * STEP_K]
            shifted = [pltpu.roll(odd[:, 128 * t : 128 * (t + 1)], 64, 1) for t in range(5)]
            for t in range(9):
                if t < 4:
                    tile = even[:, 128 * t : 128 * (t + 1)]
                elif t == 4:
                    tile = jnp.where(lane < 64, even[:, 512:640], shifted[0])
                else:
                    tile = jnp.where(lane < 64, shifted[t - 5], shifted[t - 4])
                at = pair * 2 * PIECE + 128 * t
                value = tile.reshape(per, QUARTER, 128).astype(bf16)
                out_ref[i * per : (i + 1) * per, :, at : at + 128] = value


def interpolate(k_rows, lattice, hopping):
    vmem = pl.BlockSpec(memory_space=pltpu.VMEM)
    return pl.pallas_call(
        interpolate_kernel,
        in_specs=[vmem, vmem, vmem],
        out_specs=vmem,
        out_shape=jax.ShapeDtypeStruct((GROUP, QUARTER, KEPT), bf16),
        scratch_shapes=[
            pltpu.VMEM((2 * NR, WIDE), bf16),
            pltpu.VMEM((4 * STEP_K, 2 * NR), bf16),
            pltpu.VMEM((4 * STEP_K, 2 * NR), bf16),
        ],
        compiler_params=pltpu.CompilerParams(vmem_limit_bytes=30 << 20),
        name="interpolate",
    )(k_rows, lattice, hopping)


def rotate(ut, half):
    h_re, h_im = half[:, 0:128], half[:, 128:256]
    zero = jnp.zeros((32, 256), bf16)
    rhs = jnp.concatenate(
        [half, zero, jnp.concatenate([h_im, -h_re], axis=1), zero], axis=0
    )
    full = jnp.dot(ut, rhs, preferred_element_type=f32)
    return full[:, 0:128], full[:, 128:256]


def hermitian(re, im):
    return (re + flip_square(re)) * 0.5, (im - flip_square(im)) * 0.5


def sides_kernel(column_ref, vec_ref, spin_ref, fermi_ref, wu_ref, ut_ref, sb_ref, level_ref, sp_ref):
    @pl.when(pl.program_id(0) == 0)
    def _():
        level_ref[...] = jnp.full(level_ref.shape, fermi_ref[0, 0], f32)
        sp_ref[...] = jnp.zeros_like(sp_ref)
        spin_re = spin_ref[0].astype(f32)
        spin_im = spin_ref[1].astype(f32)
        sp_ref[:, 0:WF] = ((spin_re + flip(spin_re)) * 0.5).astype(bf16)
        sp_ref[:, WF : 2 * WF] = ((spin_im - flip(spin_im)) * 0.5).astype(bf16)

    wu_ref[...] = jnp.zeros_like(wu_ref)
    ut_ref[...] = jnp.zeros_like(ut_ref)
    for q in range(SIDE_STEP):
        u_re = vec_ref[q, 0]
        u_im = vec_ref[q, 1]
        wu_ref[q, 64 : 64 + WF, 0:WF] = u_re
        wu_ref[q, 64 : 64 + WF, 128 : 128 + WF] = u_im
        wu_ref[q, 160 : 160 + WF, 0:WF] = -u_im
        wu_ref[q, 160 : 160 + WF, 128 : 128 + WF] = u_re
        ut_ref[q, :, 0:WF] = flip(u_re.astype(f32)).astype(bf16)
        ut_ref[q, :, 128 : 128 + WF] = flip(u_im.astype(f32)).astype(bf16)
    for q in range(SIDE_STEP):
        half = jnp.dot(sp_ref[...], wu_ref[q, 64:320, :], preferred_element_type=f32)
        s_re, s_im = hermitian(*rotate(ut_ref[q], half.astype(bf16)))
        sb_ref[q, :, 0:128] = s_re.astype(bf16)
        sb_ref[q, :, 128:256] = s_im.astype(bf16)


def sides(column, vectors, spin, fermi):
    per = QUARTER // SIDE_STEP
    shapes = [(320, 256), (WF, 256), (WF, 256)]
    grid_spec = pltpu.PrefetchScalarGridSpec(
        num_scalar_prefetch=1,
        grid=(per,),
        in_specs=[
            pl.BlockSpec((SIDE_STEP, 2, WF, WF), lambda i, c: (c[0] * per + i, 0, 0, 0)),
            whole((2, WF, WF)),
            pl.BlockSpec(memory_space=pltpu.SMEM),
        ],
        out_specs=[pl.BlockSpec((SIDE_STEP, *s), lambda i, c: (i, 0, 0)) for s in shapes]
        + [whole((8, 128))],
        scratch_shapes=[pltpu.VMEM((WF, 256), bf16)],
    )
    return pl.pallas_call(
        sides_kernel,
        grid_spec=grid_spec,
        out_shape=[jax.ShapeDtypeStruct((QUARTER, *s), bf16) for s in shapes]
        + [jax.ShapeDtypeStruct((8, 128), f32)],
        compiler_params=pltpu.CompilerParams(
            dimension_semantics=("arbitrary",), vmem_limit_bytes=30 << 20
        ),
        cost_estimate=pl.CostEstimate(
            flops=QUARTER * 4 * 256 * 256 * 256,
            transcendentals=0,
            bytes_accessed=QUARTER * 2 * 256 * (320 + 4 * WF),
        ),
        name="sides",
    )(column, vectors, spin, fermi)


def bands_kernel(
    wu_ref, ut_ref, sb_ref, got_ref, level_ref, curve_ref, total_ref,
    wide_ref, half_ref, bloch_ref, sum_ref,
):
    step = pl.program_id(0)

    @pl.when(step == 0)
    def _():
        for t in range(KEPT // 128):
            tile = got_ref[:, :, 128 * t : 128 * (t + 1)].astype(f32)
            for s in range(GROUP):
                wide_ref[t, PITCH * s : PITCH * s + QUARTER, :] = tile[s]
        sum_ref[...] = jnp.zeros_like(sum_ref)

    lane = lax.broadcasted_iota(jnp.int32, (WF, 128), 1)
    row = lax.broadcasted_iota(jnp.int32, (WF, 128), 0)
    eye = lane == row
    fermi = level_ref[0:1, :]
    zero = jnp.zeros((32, 256), bf16)
    mine = range(PER_STEP)

    where = {}
    for c in range(4):
        for r in range(ROWS):
            at = c * PIECE + r * 2 * WF
            odd = at % 128 != 0
            where[c, r] = (odd, 32 * sum(1 for w in where.values() if w[0] == odd), at // 128)
    for q in mine:
        k = step * PER_STEP + q
        for odd, at in ((False, 64), (True, 0)):
            rows = jnp.concatenate(
                [
                    jnp.concatenate(
                        [
                            wide_ref[w[2] + j, pl.ds(k, GROUP, stride=PITCH), :].astype(bf16)
                            for j in range(2)
                        ],
                        axis=1,
                    )
                    for w in where.values()
                    if w[0] == odd
                ],
                axis=0,
            )
            weights = wu_ref[q, at : at + 256, :]
            half = jnp.dot(rows, weights, preferred_element_type=f32).astype(bf16)
            for (c, r), w in where.items():
                if w[0] == odd:
                    half_ref[q, c, 32 * r : 32 * r + 32, :] = half[w[1] : w[1] + 32]
    for q in mine:
        for c in range(4):
            b_re, b_im = hermitian(*rotate(ut_ref[q], half_ref[q, c]))
            bloch_ref[q, c, :, 0:128] = b_re.astype(bf16)
            bloch_ref[q, c, :, 128:256] = b_im.astype(bf16)
    for q in mine:
        k = step * PER_STEP + q
        diag = jnp.where(eye, bloch_ref[q, 0, :, 0:128].astype(f32), 0.0)
        e_row = jnp.sum(diag, axis=0, keepdims=True)
        e_col = jnp.sum(diag, axis=1, keepdims=True)
        gap = e_col - e_row
        weight = -1.0 / (gap * gap + broadening * broadening)
        occupation = 1.0 / (1.0 + jnp.exp((e_row - fermi) / smearing))
        for a in range(3):
            v = bloch_ref[q, 1 + a]
            v_re, v_im = v[:, 0:128], v[:, 128:256]
            rhs = jnp.concatenate(
                [v, zero, jnp.concatenate([-v_im, v_re], axis=1), zero], axis=0
            )
            prod = jnp.dot(sb_ref[q], rhs, preferred_element_type=f32)
            p_re = prod[:, 0:128]
            p_im = prod[:, 128:256]
            c_re = (p_re + flip_square(p_re)) * weight
            c_im = (p_im - flip_square(p_im)) * weight
            for b in range(3):
                w_re = bloch_ref[q, 1 + b, :, 0:128].astype(f32)
                w_im = bloch_ref[q, 1 + b, :, 128:256].astype(f32)
                curve = jnp.sum(c_re * w_im - c_im * w_re, axis=0, keepdims=True)
                curve_ref[3 * a + b, pl.ds(k, 1), :] = curve[:, 0:WF]
                sum_ref[3 * a + b : 3 * a + b + 1, :] += occupation * curve

    @pl.when(step == pl.num_programs(0) - 1)
    def _():
        last = jnp.broadcast_to(sum_ref[8:9, :], (8, 128))
        lane8 = lax.broadcasted_iota(jnp.int32, (8, 128), 1)
        row8 = lax.broadcasted_iota(jnp.int32, (8, 128), 0)
        extra = jnp.zeros((8, 128), f32)
        for t in range(3):
            extra = jnp.where(row8 == t, pltpu.roll(last, 96 - 32 * t, 1), extra)
        packed = jnp.where(lane8 < WF, sum_ref[0:8, :], extra)
        total_ref[...] = jnp.broadcast_to(packed[None], total_ref.shape)


def bands(count, prepared, got, level):
    per = QUARTER // PER_STEP
    shapes = [(9, QUARTER, WF), (count, 8, 128)]
    return pl.pallas_call(
        bands_kernel,
        grid=(per,),
        in_specs=[
            pl.BlockSpec((PER_STEP, *p.shape[1:]), lambda i: (i, 0, 0)) for p in prepared
        ]
        + [pl.BlockSpec(memory_space=pltpu.VMEM)] * 2,
        out_specs=[pl.BlockSpec(memory_space=pltpu.VMEM) for _ in shapes],
        out_shape=[jax.ShapeDtypeStruct(shape, f32) for shape in shapes],
        scratch_shapes=[
            pltpu.VMEM((KEPT // 128, GROUP * PITCH, 128), f32),
            pltpu.VMEM((PER_STEP, 4, WF, 256), bf16),
            pltpu.VMEM((PER_STEP, 4, WF, 256), bf16),
            pltpu.VMEM((16, 128), f32),
        ],
        compiler_params=pltpu.CompilerParams(
            dimension_semantics=("arbitrary",), vmem_limit_bytes=30 << 20
        ),
        name="bands",
    )(*prepared, got, level)


def exchange(value, axes):
    return lax.all_to_all(value, axes, split_axis=0, concat_axis=0, tiled=True)


def on_device(hamiltonian, eigvecs, spin, k_indices, r_vectors, degeneracy, fermi_level):
    own = hamiltonian.shape[0]
    pieces = hamiltonian.reshape(own, 2, ROWS, GROUP, WF).transpose(3, 0, 2, 1, 4)
    pieces = pieces.reshape(GROUP, own, PIECE)
    points = jnp.zeros((own, WIDE - PIECE), bf16).at[0:3, :].set(k_indices.T.astype(bf16))
    points = jnp.broadcast_to(points[None], (GROUP, own, WIDE - PIECE))
    pieces = jnp.concatenate([pieces, points], axis=2)
    pieces = jnp.broadcast_to(pieces[None], (4, GROUP, own, WIDE)).reshape(4 * GROUP, own, WIDE)
    hopping = exchange(pieces, ALL)
    column = lax.axis_index("x").astype(jnp.int32).reshape(1)
    vectors = pltpu.with_memory_space_constraint(eigvecs, pltpu.HBM)
    *prepared, level = sides(column, vectors, spin, fermi_level.reshape(1, 1))
    prepared = [pltpu.with_memory_space_constraint(p, pltpu.HBM) for p in prepared]
    layer = lax.axis_index("z")
    mine = lax.dynamic_slice(hopping, (layer * GROUP, 0, 0), (GROUP, own, WIDE))
    k_rows = mine.reshape(8, 4, own, WIDE)[:, 0, :, PIECE:]
    k_rows = k_rows.transpose(0, 2, 1).reshape(8 * (WIDE - PIECE), own).astype(f32)
    lattice = jnp.concatenate(
        [r_vectors.T.astype(f32), jnp.broadcast_to(degeneracy.astype(f32)[None], (5, NR))], axis=0
    )
    entries = interpolate(k_rows, lattice, hopping.reshape(NR, WIDE))
    entries, level, *prepared = lax.optimization_barrier((entries, level, *prepared))
    got = exchange(entries, PLANE)
    count = lax.axis_size("z") * lax.axis_size("y") * lax.axis_size("core") * lax.axis_size("x")
    curvature, copies = bands(count, prepared, got, level)
    total_points = k_indices.shape[0] * count // 4
    total = jnp.sum(exchange(copies, ALL), axis=0) * (1.0 / math.sqrt(total_points))
    last = total[0:3, WF:].reshape(1, WF)
    totals = jnp.concatenate([total[:, :WF], last], axis=0)
    return (curvature.transpose(0, 2, 1), totals)


def solution(mesh):
    fine = Mesh(mesh.devices.reshape(4, 4, 2, 4), ALL)
    ka = ("z", "y", "core")
    in_specs = (P(ALL, None, None), P(ka, None, None, None), P(), P(ka, None), P(), P(), P())
    out_specs = (P(None, None, ALL), P())
    return jax.shard_map(
        on_device, mesh=fine, in_specs=in_specs, out_specs=out_specs, check_vma=False
    )
```

```python
import math

import jax
import jax.numpy as jnp
from jax import lax
from jax.experimental import pallas as pl
from jax.experimental.pallas import tpu as pltpu
from jax.sharding import Mesh, PartitionSpec as P

WF = 96
GRID = 64
NR = 1024
GROUP = 32
ROWS = 3
PIECE = ROWS * 2 * WF
WIDE = 640
KEPT = 4 * PIECE
QUARTER = 16
PITCH = 17
STEP_K = 128
PER_STEP = 4
SIDE_STEP = 4

broadening = 0.5
smearing = 0.1

ALL = ("z", "y", "core", "x")
PLANE = ("y", "core", "x")

f32 = jnp.float32
bf16 = jnp.bfloat16

SINE = (3.14159264, -5.16771009, 2.55007766, -0.59829216, 0.07765941)
COSINE = (0.99999995, -4.93479286, 4.05841192, -1.33188016, 0.2196968)


def whole(shape):
    return pl.BlockSpec(shape, lambda *_: (0,) * len(shape))


def horner(coefficients, q):
    value = coefficients[-1]
    for c in coefficients[-2::-1]:
        value = value * q + c
    return value


def turn(f):
    q = f * f
    s = f * horner(SINE, q)
    twice = s + s
    return 1.0 - twice * s, twice * horner(COSINE, q)


def flip(x):
    return jnp.transpose(x, (1, 0))


def flip_square(x):
    pad = jnp.zeros((32, 128), f32)
    return flip(jnp.concatenate([x, pad], axis=0))[0:WF]


def pack_kernel(ham_ref, k_ref, out_ref, piece_ref, points_ref, sems):
    lane = lax.broadcasted_iota(jnp.int32, (8, 128), 1)
    points_ref[...] = jnp.zeros_like(points_ref)
    points_ref[0:3, 64:128] = k_ref[...].astype(f32)
    points = points_ref[...]
    loaded = {}

    def tile(part, t):
        if (part, t) not in loaded:
            loaded[part, t] = ham_ref[:, part, 128 * t : 128 * (t + 1)].astype(f32)
        return loaded[part, t]

    def segment(part, line, start, size, at):
        first = WF * line + start
        shift = (at - first) % 128
        move = lambda t: pltpu.roll(tile(part, t), shift, 1) if shift else tile(part, t)
        value = move(first // 128)
        if (first + size - 1) // 128 != first // 128:
            cut = at + 128 - first % 128
            value = jnp.where(lane < cut, value, move(first // 128 + 1))
        return value

    layout = [
        ((0, 0, 0, 96, 0), (1, 0, 0, 32, 96)),
        ((1, 0, 32, 64, 0), (0, 1, 0, 64, 64)),
        ((0, 1, 64, 32, 0), (1, 1, 0, 96, 32)),
        ((0, 2, 0, 96, 0), (1, 2, 0, 32, 96)),
        ((1, 2, 32, 64, 0), None),
    ]
    for g in range(GROUP):
        for t, (left, right) in enumerate(layout):
            part, r, start, size, at = left
            value = segment(part, GROUP * r + g, start, size, at)
            if right is None:
                other = points
            else:
                other = segment(right[0], GROUP * right[1] + g, *right[2:])
            value = jnp.where(lane < size, value, other)
            piece_ref[g, :, 128 * t : 128 * (t + 1)] = value.astype(bf16)
    layers = out_ref.shape[0] // GROUP
    copies = [
        pltpu.make_async_copy(piece_ref, out_ref.at[pl.ds(GROUP * z, GROUP)], sems.at[z])
        for z in range(layers)
    ]
    for copy in copies:
        copy.start()
    for copy in copies:
        copy.wait()


def pack(hamiltonian, k_rows, count):
    own = hamiltonian.shape[0]
    vmem = pl.BlockSpec(memory_space=pltpu.VMEM)
    return pl.pallas_call(
        pack_kernel,
        in_specs=[vmem, vmem],
        out_specs=pl.BlockSpec(memory_space=pl.ANY),
        out_shape=jax.ShapeDtypeStruct((count, own, WIDE), bf16),
        scratch_shapes=[
            pltpu.VMEM((GROUP, own, WIDE), bf16),
            pltpu.VMEM((8, 128), f32),
            pltpu.SemaphoreType.DMA((count // GROUP,)),
        ],
        name="pack",
    )(hamiltonian, k_rows)


def turn_hopping(hop_ref, w_ref):
    lane = lax.broadcasted_iota(jnp.int32, (NR, 128), 1)
    tiles = [hop_ref[:, 128 * t : 128 * (t + 1)].astype(f32) for t in range(5)]
    tiles[4] = jnp.where(lane < 64, tiles[4], 0.0)
    ups = [pltpu.roll(t, 96, 1) for t in tiles]
    downs = [pltpu.roll(t, 32, 1) for t in tiles]
    for t in range(5):
        w_ref[0:NR, 128 * t : 128 * (t + 1)] = tiles[t].astype(bf16)
        up = jnp.where(lane < 96, ups[(t - 1) % 5], ups[t])
        down = jnp.where(lane < 32, downs[t], downs[(t + 1) % 5])
        place = (lane + 128 * t) % (2 * WF)
        turned = jnp.where(place < WF, -down, up)
        if t == 4:
            turned = jnp.where(lane < 64, turned, 0.0)
        w_ref[NR : 2 * NR, 128 * t : 128 * (t + 1)] = turned.astype(bf16)


def phase_block(k, lat_ref, p_ref):
    r = [lat_ref[a : a + 1, :] for a in range(3)]
    inverse = 1.0 / lat_ref[3:4, :]
    turns = sum(k[:, a : a + 1] * (r[a] * (1.0 / GRID)) for a in range(3))
    cosine, sine = turn(turns - jnp.floor(turns + 0.5))
    for c in range(4):
        rows = slice(c * STEP_K, (c + 1) * STEP_K)
        if c == 0:
            re, im = cosine * inverse, sine * inverse
        else:
            coord = r[c - 1] * inverse
            re, im = sine * (-coord), cosine * coord
        p_ref[rows, 0:NR] = re.astype(bf16)
        p_ref[rows, NR : 2 * NR] = im.astype(bf16)


def interpolate_kernel(k_ref, lat_ref, hop_ref, out_ref, w_ref, *p_refs):
    steps = GROUP * QUARTER // STEP_K
    per = STEP_K // QUARTER
    lane = lax.broadcasted_iota(jnp.int32, (STEP_K, 128), 1)

    def phases(i):
        phase_block(k_ref[i * STEP_K : (i + 1) * STEP_K, :], lat_ref, p_refs[i % 2])

    phases(0)
    turn_hopping(hop_ref, w_ref)
    for i in range(steps):
        if i + 1 < steps:
            phases(i + 1)
        summed = jnp.dot(p_refs[i % 2][...], w_ref[...], preferred_element_type=f32)
        for pair in range(2):
            even = summed[2 * pair * STEP_K : (2 * pair + 1) * STEP_K]
            odd = summed[(2 * pair + 1) * STEP_K : (2 * pair + 2) * STEP_K]
            shifted = [pltpu.roll(odd[:, 128 * t : 128 * (t + 1)], 64, 1) for t in range(5)]
            for t in range(9):
                if t < 4:
                    tile = even[:, 128 * t : 128 * (t + 1)]
                elif t == 4:
                    tile = jnp.where(lane < 64, even[:, 512:640], shifted[0])
                else:
                    tile = jnp.where(lane < 64, shifted[t - 5], shifted[t - 4])
                at = pair * 2 * PIECE + 128 * t
                value = tile.reshape(per, QUARTER, 128).astype(bf16)
                out_ref[i * per : (i + 1) * per, :, at : at + 128] = value


def interpolate(k_rows, lattice, hopping):
    vmem = pl.BlockSpec(memory_space=pltpu.VMEM)
    return pl.pallas_call(
        interpolate_kernel,
        in_specs=[vmem, vmem, vmem],
        out_specs=vmem,
        out_shape=jax.ShapeDtypeStruct((GROUP, QUARTER, KEPT), bf16),
        scratch_shapes=[
            pltpu.VMEM((2 * NR, WIDE), bf16),
            pltpu.VMEM((4 * STEP_K, 2 * NR), bf16),
            pltpu.VMEM((4 * STEP_K, 2 * NR), bf16),
        ],
        compiler_params=pltpu.CompilerParams(vmem_limit_bytes=30 << 20),
        name="interpolate",
    )(k_rows, lattice, hopping)


def rotate(ut, half):
    h_re, h_im = half[:, 0:128], half[:, 128:256]
    zero = jnp.zeros((32, 256), bf16)
    rhs = jnp.concatenate(
        [half, zero, jnp.concatenate([h_im, -h_re], axis=1), zero], axis=0
    )
    full = jnp.dot(ut, rhs, preferred_element_type=f32)
    return full[:, 0:128], full[:, 128:256]


def hermitian(re, im):
    return (re + flip_square(re)) * 0.5, (im - flip_square(im)) * 0.5


def sides_kernel(column_ref, vec_ref, spin_ref, fermi_ref, wu_ref, ut_ref, sb_ref, level_ref, sp_ref):
    @pl.when(pl.program_id(0) == 0)
    def _():
        level_ref[...] = jnp.full(level_ref.shape, fermi_ref[0, 0], f32)
        sp_ref[...] = jnp.zeros_like(sp_ref)
        spin_re = spin_ref[0].astype(f32)
        spin_im = spin_ref[1].astype(f32)
        sp_ref[:, 0:WF] = ((spin_re + flip(spin_re)) * 0.5).astype(bf16)
        sp_ref[:, WF : 2 * WF] = ((spin_im - flip(spin_im)) * 0.5).astype(bf16)

    wu_ref[...] = jnp.zeros_like(wu_ref)
    ut_ref[...] = jnp.zeros_like(ut_ref)
    for q in range(SIDE_STEP):
        u_re = vec_ref[q, 0]
        u_im = vec_ref[q, 1]
        wu_ref[q, 64 : 64 + WF, 0:WF] = u_re
        wu_ref[q, 64 : 64 + WF, 128 : 128 + WF] = u_im
        wu_ref[q, 160 : 160 + WF, 0:WF] = -u_im
        wu_ref[q, 160 : 160 + WF, 128 : 128 + WF] = u_re
        ut_ref[q, :, 0:WF] = flip(u_re.astype(f32)).astype(bf16)
        ut_ref[q, :, 128 : 128 + WF] = flip(u_im.astype(f32)).astype(bf16)
    for q in range(SIDE_STEP):
        half = jnp.dot(sp_ref[...], wu_ref[q, 64:320, :], preferred_element_type=f32)
        s_re, s_im = hermitian(*rotate(ut_ref[q], half.astype(bf16)))
        sb_ref[q, :, 0:128] = s_re.astype(bf16)
        sb_ref[q, :, 128:256] = s_im.astype(bf16)


def sides(column, vectors, spin, fermi):
    per = QUARTER // SIDE_STEP
    shapes = [(320, 256), (WF, 256), (WF, 256)]
    grid_spec = pltpu.PrefetchScalarGridSpec(
        num_scalar_prefetch=1,
        grid=(per,),
        in_specs=[
            pl.BlockSpec((SIDE_STEP, 2, WF, WF), lambda i, c: (c[0] * per + i, 0, 0, 0)),
            whole((2, WF, WF)),
            pl.BlockSpec(memory_space=pltpu.SMEM),
        ],
        out_specs=[pl.BlockSpec((SIDE_STEP, *s), lambda i, c: (i, 0, 0)) for s in shapes]
        + [whole((8, 128))],
        scratch_shapes=[pltpu.VMEM((WF, 256), bf16)],
    )
    return pl.pallas_call(
        sides_kernel,
        grid_spec=grid_spec,
        out_shape=[jax.ShapeDtypeStruct((QUARTER, *s), bf16) for s in shapes]
        + [jax.ShapeDtypeStruct((8, 128), f32)],
        compiler_params=pltpu.CompilerParams(
            dimension_semantics=("arbitrary",), vmem_limit_bytes=30 << 20
        ),
        cost_estimate=pl.CostEstimate(
            flops=QUARTER * 4 * 256 * 256 * 256,
            transcendentals=0,
            bytes_accessed=QUARTER * 2 * 256 * (320 + 4 * WF),
        ),
        name="sides",
    )(column, vectors, spin, fermi)


def bands_kernel(
    wu_ref, ut_ref, sb_ref, got_ref, level_ref, curve_ref, total_ref,
    wide_ref, half_ref, *bloch_refs,
):
    for t in range(KEPT // 128):
        tile = got_ref[:, :, 128 * t : 128 * (t + 1)].astype(f32)
        for s in range(GROUP):
            wide_ref[t, PITCH * s : PITCH * s + QUARTER, :] = tile[s]

    lane = lax.broadcasted_iota(jnp.int32, (WF, 128), 1)
    row = lax.broadcasted_iota(jnp.int32, (WF, 128), 0)
    eye = lane == row
    fermi = level_ref[0:1, :]
    zero = jnp.zeros((32, 256), bf16)

    where = {}
    for c in range(4):
        for r in range(ROWS):
            at = c * PIECE + r * 2 * WF
            odd = at % 128 != 0
            where[c, r] = (odd, 32 * sum(1 for w in where.values() if w[0] == odd), at // 128)

    def first_product(k, slot):
        for odd, at in ((False, 64), (True, 0)):
            rows = jnp.concatenate(
                [
                    jnp.concatenate(
                        [
                            wide_ref[w[2] + j, pl.ds(k, GROUP, stride=PITCH), :].astype(bf16)
                            for j in range(2)
                        ],
                        axis=1,
                    )
                    for w in where.values()
                    if w[0] == odd
                ],
                axis=0,
            )
            weights = wu_ref[k, at : at + 256, :]
            half = jnp.dot(rows, weights, preferred_element_type=f32).astype(bf16)
            for (c, r), w in where.items():
                if w[0] == odd:
                    half_ref[slot, c, 32 * r : 32 * r + 32, :] = half[w[1] : w[1] + 32]

    def second_product(k, slot, bloch_ref):
        for c in range(4):
            b_re, b_im = hermitian(*rotate(ut_ref[k], half_ref[slot, c]))
            bloch_ref[c, :, 0:128] = b_re.astype(bf16)
            bloch_ref[c, :, 128:256] = b_im.astype(bf16)

    sums = [jnp.zeros((1, 128), f32) for _ in range(9)]

    def kubo(k, bloch_ref):
        diag = jnp.where(eye, bloch_ref[0, :, 0:128].astype(f32), 0.0)
        e_row = jnp.sum(diag, axis=0, keepdims=True)
        e_col = jnp.sum(diag, axis=1, keepdims=True)
        gap = e_col - e_row
        weight = -1.0 / (gap * gap + broadening * broadening)
        occupation = 1.0 / (1.0 + jnp.exp((e_row - fermi) / smearing))
        for a in range(3):
            v = bloch_ref[1 + a]
            v_re, v_im = v[:, 0:128], v[:, 128:256]
            rhs = jnp.concatenate(
                [v, zero, jnp.concatenate([-v_im, v_re], axis=1), zero], axis=0
            )
            prod = jnp.dot(sb_ref[k], rhs, preferred_element_type=f32)
            p_re = prod[:, 0:128]
            p_im = prod[:, 128:256]
            c_re = (p_re + flip_square(p_re)) * weight
            c_im = (p_im - flip_square(p_im)) * weight
            for b in range(3):
                w_re = bloch_ref[1 + b, :, 0:128].astype(f32)
                w_im = bloch_ref[1 + b, :, 128:256].astype(f32)
                curve = jnp.sum(c_re * w_im - c_im * w_re, axis=0, keepdims=True)
                curve_ref[3 * a + b, k : k + 1, :] = curve[:, 0:WF]
                sums[3 * a + b] = sums[3 * a + b] + occupation * curve

    steps = QUARTER // PER_STEP
    for i in range(steps + 1):
        for q in range(PER_STEP):
            if i < steps:
                first_product(i * PER_STEP + q, i % 2 * PER_STEP + q)
        for q in range(PER_STEP):
            if i > 0:
                kubo((i - 1) * PER_STEP + q, bloch_refs[(i - 1) % 2 * PER_STEP + q])
            if i < steps:
                slot = i % 2 * PER_STEP + q
                second_product(i * PER_STEP + q, slot, bloch_refs[slot])

    lane8 = lax.broadcasted_iota(jnp.int32, (8, 128), 1)
    row8 = lax.broadcasted_iota(jnp.int32, (8, 128), 0)
    packed = jnp.zeros((8, 128), f32)
    for ab in range(8):
        packed = jnp.where(row8 == ab, sums[ab], packed)
    last = jnp.broadcast_to(sums[8], (8, 128))
    for t in range(3):
        moved = pltpu.roll(last, 96 - 32 * t, 1)
        packed = jnp.where((lane8 >= WF) & (row8 == t), moved, packed)
    total_ref[...] = jnp.broadcast_to(packed[None], total_ref.shape)


def bands(count, prepared, got, level):
    shapes = [(9, QUARTER, WF), (count, 8, 128)]
    vmem = pl.BlockSpec(memory_space=pltpu.VMEM)
    return pl.pallas_call(
        bands_kernel,
        in_specs=[vmem] * 5,
        out_specs=[vmem] * 2,
        out_shape=[jax.ShapeDtypeStruct(shape, f32) for shape in shapes],
        scratch_shapes=[
            pltpu.VMEM((KEPT // 128, GROUP * PITCH, 128), f32),
            pltpu.VMEM((2 * PER_STEP, 4, WF, 256), bf16),
        ]
        + [pltpu.VMEM((4, WF, 256), bf16)] * (2 * PER_STEP),
        compiler_params=pltpu.CompilerParams(vmem_limit_bytes=30 << 20),
        name="bands",
    )(*prepared, got, level)


def exchange(value, axes):
    return lax.all_to_all(value, axes, split_axis=0, concat_axis=0, tiled=True)


def on_device(hamiltonian, eigvecs, spin, k_indices, r_vectors, degeneracy, fermi_level):
    own = hamiltonian.shape[0]
    count = lax.axis_size("z") * lax.axis_size("y") * lax.axis_size("core") * lax.axis_size("x")
    pieces = pack(hamiltonian, k_indices.T, count)
    hopping = exchange(pieces, ALL)
    column = lax.axis_index("x").astype(jnp.int32).reshape(1)
    vectors = pltpu.with_memory_space_constraint(eigvecs, pltpu.HBM)
    *prepared, level = sides(column, vectors, spin, fermi_level.reshape(1, 1))
    layer = lax.axis_index("z")
    mine = lax.dynamic_slice(hopping, (layer * GROUP, 0, 0), (GROUP, own, WIDE))
    k_rows = mine.reshape(8, 4, own, WIDE)[:, 0, :, PIECE:]
    k_rows = k_rows.transpose(0, 2, 1).reshape(8 * (WIDE - PIECE), own).astype(f32)
    lattice = jnp.concatenate(
        [r_vectors.T.astype(f32), jnp.broadcast_to(degeneracy.astype(f32)[None], (5, NR))], axis=0
    )
    entries = interpolate(k_rows, lattice, hopping.reshape(NR, WIDE))
    entries, level, *prepared = lax.optimization_barrier((entries, level, *prepared))
    got = exchange(entries, PLANE)
    curvature, copies = bands(count, prepared, got, level)
    total_points = k_indices.shape[0] * count // 4
    total = jnp.sum(exchange(copies, ALL), axis=0) * (1.0 / math.sqrt(total_points))
    last = total[0:3, WF:].reshape(1, WF)
    totals = jnp.concatenate([total[:, :WF], last], axis=0)
    return (curvature.transpose(0, 2, 1), totals)


def solution(mesh):
    fine = Mesh(mesh.devices.reshape(4, 4, 2, 4), ALL)
    ka = ("z", "y", "core")
    in_specs = (P(ALL, None, None), P(ka, None, None, None), P(), P(ka, None), P(), P(), P())
    out_specs = (P(None, None, ALL), P())
    return jax.shard_map(
        on_device, mesh=fine, in_specs=in_specs, out_specs=out_specs, check_vma=False
    )
```

```python
import math

import jax
import jax.numpy as jnp
from jax import lax
from jax.experimental import pallas as pl
from jax.experimental.pallas import tpu as pltpu
from jax.sharding import Mesh, PartitionSpec as P

WF = 96
GRID = 64
NR = 1024
GROUP = 32
ROWS = 3
PIECE = ROWS * 2 * WF
WIDE = 640
KEPT = 4 * PIECE
QUARTER = 16
PITCH = 17
STEP_K = 128
PER_STEP = 4
SIDE_STEP = 4

broadening = 0.5
smearing = 0.1

ALL = ("z", "y", "core", "x")
PLANE = ("y", "core", "x")

f32 = jnp.float32
bf16 = jnp.bfloat16

SINE = (3.14159264, -5.16771009, 2.55007766, -0.59829216, 0.07765941)
COSINE = (0.99999995, -4.93479286, 4.05841192, -1.33188016, 0.2196968)


def whole(shape):
    return pl.BlockSpec(shape, lambda *_: (0,) * len(shape))


def horner(coefficients, q):
    value = coefficients[-1]
    for c in coefficients[-2::-1]:
        value = value * q + c
    return value


def turn(f):
    q = f * f
    s = f * horner(SINE, q)
    twice = s + s
    return 1.0 - twice * s, twice * horner(COSINE, q)


def flip(x):
    return jnp.transpose(x, (1, 0))


def flip_square(x):
    pad = jnp.zeros((32, 128), f32)
    return flip(jnp.concatenate([x, pad], axis=0))[0:WF]


def pack_kernel(ham_ref, k_ref, out_ref, piece_ref, points_ref, sems):
    lane = lax.broadcasted_iota(jnp.int32, (8, 128), 1)
    points_ref[...] = jnp.zeros_like(points_ref)
    points_ref[0:3, 64:128] = k_ref[...].astype(f32)
    points = points_ref[...]
    loaded = {}
    copies = []

    def tile(part, t):
        if (part, t) not in loaded:
            loaded[part, t] = ham_ref[:, part, 128 * t : 128 * (t + 1)].astype(f32)
        return loaded[part, t]

    def segment(part, line, start, size, at):
        first = WF * line + start
        shift = (at - first) % 128
        move = lambda t: pltpu.roll(tile(part, t), shift, 1) if shift else tile(part, t)
        value = move(first // 128)
        if (first + size - 1) // 128 != first // 128:
            cut = at + 128 - first % 128
            value = jnp.where(lane < cut, value, move(first // 128 + 1))
        return value

    layout = [
        ((0, 0, 0, 96, 0), (1, 0, 0, 32, 96)),
        ((1, 0, 32, 64, 0), (0, 1, 0, 64, 64)),
        ((0, 1, 64, 32, 0), (1, 1, 0, 96, 32)),
        ((0, 2, 0, 96, 0), (1, 2, 0, 32, 96)),
        ((1, 2, 32, 64, 0), None),
    ]
    for g in range(GROUP):
        for t, (left, right) in enumerate(layout):
            part, r, start, size, at = left
            value = segment(part, GROUP * r + g, start, size, at)
            if right is None:
                other = points
            else:
                other = segment(right[0], GROUP * right[1] + g, *right[2:])
            value = jnp.where(lane < size, value, other)
            piece_ref[g, :, 128 * t : 128 * (t + 1)] = value.astype(bf16)
        if g % 8 == 7:
            for z in range(out_ref.shape[0] // GROUP):
                copies.append(
                    pltpu.make_async_copy(
                        piece_ref.at[pl.ds(g - 7, 8)],
                        out_ref.at[pl.ds(GROUP * z + g - 7, 8)],
                        sems.at[g // 8, z],
                    )
                )
                copies[-1].start()
    for copy in copies:
        copy.wait()


def pack(hamiltonian, k_rows, count):
    own = hamiltonian.shape[0]
    vmem = pl.BlockSpec(memory_space=pltpu.VMEM)
    return pl.pallas_call(
        pack_kernel,
        in_specs=[vmem, vmem],
        out_specs=pl.BlockSpec(memory_space=pl.ANY),
        out_shape=jax.ShapeDtypeStruct((count, own, WIDE), bf16),
        scratch_shapes=[
            pltpu.VMEM((GROUP, own, WIDE), bf16),
            pltpu.VMEM((8, 128), f32),
            pltpu.SemaphoreType.DMA((4, count // GROUP)),
        ],
        name="pack",
    )(hamiltonian, k_rows)


def turn_hopping(hop_ref, w_ref):
    lane = lax.broadcasted_iota(jnp.int32, (NR, 128), 1)
    tiles = [hop_ref[:, 128 * t : 128 * (t + 1)].astype(f32) for t in range(5)]
    ups = [pltpu.roll(t, 96, 1) for t in tiles]
    downs = [pltpu.roll(t, 32, 1) for t in tiles]
    for t in range(5):
        up = jnp.where(lane < 96, ups[(t - 1) % 5], ups[t])
        down = jnp.where(lane < 32, downs[t], downs[(t + 1) % 5])
        place = (lane + 128 * t) % (2 * WF)
        turned = jnp.where(place < WF, -down, up)
        w_ref[:, 128 * t : 128 * (t + 1)] = turned.astype(bf16)


def phase_block(k, lat_ref, p_ref):
    r = [lat_ref[a : a + 1, :] for a in range(3)]
    inverse = 1.0 / lat_ref[3:4, :]
    turns = jnp.dot(
        k.astype(bf16), (lat_ref[...] * (1.0 / GRID)).astype(bf16), preferred_element_type=f32
    )
    cosine, sine = turn(turns - jnp.floor(turns + 0.5))
    for c in range(4):
        rows = slice(c * STEP_K, (c + 1) * STEP_K)
        if c == 0:
            re, im = cosine * inverse, sine * inverse
        else:
            coord = r[c - 1] * inverse
            re, im = sine * (-coord), cosine * coord
        p_ref[rows, 0:NR] = re.astype(bf16)
        p_ref[rows, NR : 2 * NR] = im.astype(bf16)


def interpolate_kernel(k_ref, lat_ref, hop_ref, out_ref, w_ref, *p_refs):
    steps = GROUP * QUARTER // STEP_K
    per = STEP_K // QUARTER
    lane = lax.broadcasted_iota(jnp.int32, (STEP_K, 128), 1)

    def phases(i):
        phase_block(k_ref[i * STEP_K : (i + 1) * STEP_K, :], lat_ref, p_refs[i % 2])

    phases(0)
    turn_hopping(hop_ref, w_ref)
    for i in range(steps):
        if i + 1 < steps:
            phases(i + 1)
        p_ref = p_refs[i % 2]
        summed = jnp.dot(p_ref[:, 0:NR], hop_ref[...], preferred_element_type=f32)
        summed += jnp.dot(p_ref[:, NR : 2 * NR], w_ref[...], preferred_element_type=f32)
        for pair in range(2):
            even = summed[2 * pair * STEP_K : (2 * pair + 1) * STEP_K]
            odd = summed[(2 * pair + 1) * STEP_K : (2 * pair + 2) * STEP_K]
            shifted = [pltpu.roll(odd[:, 128 * t : 128 * (t + 1)], 64, 1) for t in range(5)]
            for t in range(9):
                if t < 4:
                    tile = even[:, 128 * t : 128 * (t + 1)]
                elif t == 4:
                    tile = jnp.where(lane < 64, even[:, 512:640], shifted[0])
                else:
                    tile = jnp.where(lane < 64, shifted[t - 5], shifted[t - 4])
                at = pair * 2 * PIECE + 128 * t
                value = tile.reshape(per, QUARTER, 128).astype(bf16)
                out_ref[i * per : (i + 1) * per, :, at : at + 128] = value


def interpolate(k_rows, lattice, hopping):
    vmem = pl.BlockSpec(memory_space=pltpu.VMEM)
    return pl.pallas_call(
        interpolate_kernel,
        in_specs=[vmem, vmem, vmem],
        out_specs=vmem,
        out_shape=jax.ShapeDtypeStruct((GROUP, QUARTER, KEPT), bf16),
        scratch_shapes=[
            pltpu.VMEM((NR, WIDE), bf16),
            pltpu.VMEM((4 * STEP_K, 2 * NR), bf16),
            pltpu.VMEM((4 * STEP_K, 2 * NR), bf16),
        ],
        compiler_params=pltpu.CompilerParams(vmem_limit_bytes=30 << 20),
        name="interpolate",
    )(k_rows, lattice, hopping)


def rotate(ut, half):
    h_re, h_im = half[:, 0:128], half[:, 128:256]
    zero = jnp.zeros((32, 256), bf16)
    rhs = jnp.concatenate(
        [half, zero, jnp.concatenate([h_im, -h_re], axis=1), zero], axis=0
    )
    full = jnp.dot(ut, rhs, preferred_element_type=f32)
    return full[:, 0:128], full[:, 128:256]


def hermitian(re, im):
    return (re + flip_square(re)) * 0.5, (im - flip_square(im)) * 0.5


def sides_kernel(column_ref, vec_ref, spin_ref, fermi_ref, wu_ref, ut_ref, sb_ref, level_ref, sp_ref):
    @pl.when(pl.program_id(0) == 0)
    def _():
        level_ref[...] = jnp.full(level_ref.shape, fermi_ref[0, 0], f32)
        sp_ref[...] = jnp.zeros_like(sp_ref)
        spin_re = spin_ref[0].astype(f32)
        spin_im = spin_ref[1].astype(f32)
        sp_ref[:, 0:WF] = ((spin_re + flip(spin_re)) * 0.5).astype(bf16)
        sp_ref[:, WF : 2 * WF] = ((spin_im - flip(spin_im)) * 0.5).astype(bf16)

    wu_ref[...] = jnp.zeros_like(wu_ref)
    ut_ref[...] = jnp.zeros_like(ut_ref)
    for q in range(SIDE_STEP):
        u_re = vec_ref[q, 0]
        u_im = vec_ref[q, 1]
        wu_ref[q, 64 : 64 + WF, 0:WF] = u_re
        wu_ref[q, 64 : 64 + WF, 128 : 128 + WF] = u_im
        wu_ref[q, 160 : 160 + WF, 0:WF] = -u_im
        wu_ref[q, 160 : 160 + WF, 128 : 128 + WF] = u_re
        ut_ref[q, :, 0:WF] = flip(u_re.astype(f32)).astype(bf16)
        ut_ref[q, :, 128 : 128 + WF] = flip(u_im.astype(f32)).astype(bf16)
    for q in range(SIDE_STEP):
        half = jnp.dot(sp_ref[...], wu_ref[q, 64:320, :], preferred_element_type=f32)
        s_re, s_im = hermitian(*rotate(ut_ref[q], half.astype(bf16)))
        sb_ref[q, :, 0:128] = s_re.astype(bf16)
        sb_ref[q, :, 128:256] = s_im.astype(bf16)


def sides(column, vectors, spin, fermi):
    per = QUARTER // SIDE_STEP
    shapes = [(320, 256), (WF, 256), (WF, 256)]
    grid_spec = pltpu.PrefetchScalarGridSpec(
        num_scalar_prefetch=1,
        grid=(per,),
        in_specs=[
            pl.BlockSpec((SIDE_STEP, 2, WF, WF), lambda i, c: (c[0] * per + i, 0, 0, 0)),
            whole((2, WF, WF)),
            pl.BlockSpec(memory_space=pltpu.SMEM),
        ],
        out_specs=[pl.BlockSpec((SIDE_STEP, *s), lambda i, c: (i, 0, 0)) for s in shapes]
        + [whole((8, 128))],
        scratch_shapes=[pltpu.VMEM((WF, 256), bf16)],
    )
    return pl.pallas_call(
        sides_kernel,
        grid_spec=grid_spec,
        out_shape=[jax.ShapeDtypeStruct((QUARTER, *s), bf16) for s in shapes]
        + [jax.ShapeDtypeStruct((8, 128), f32)],
        compiler_params=pltpu.CompilerParams(
            dimension_semantics=("arbitrary",), vmem_limit_bytes=30 << 20
        ),
        cost_estimate=pl.CostEstimate(
            flops=QUARTER * 4 * 256 * 256 * 256,
            transcendentals=0,
            bytes_accessed=QUARTER * 2 * 256 * (320 + 4 * WF),
        ),
        name="sides",
    )(column, vectors, spin, fermi)


def bands_kernel(
    wu_ref, ut_ref, sb_ref, got_ref, level_ref, curve_ref, total_ref,
    wide_ref, half_ref, *others,
):
    bloch_refs, flow_refs = others[: 2 * PER_STEP], others[2 * PER_STEP :]
    for t in range(KEPT // 128):
        tile = got_ref[:, :, 128 * t : 128 * (t + 1)].astype(f32)
        for s in range(GROUP):
            wide_ref[t, PITCH * s : PITCH * s + QUARTER, :] = tile[s]

    lane = lax.broadcasted_iota(jnp.int32, (WF, 128), 1)
    row = lax.broadcasted_iota(jnp.int32, (WF, 128), 0)
    eye = lane == row
    fermi = level_ref[0:1, :]
    zero = jnp.zeros((32, 256), bf16)

    where = {}
    for c in range(4):
        for r in range(ROWS):
            at = c * PIECE + r * 2 * WF
            odd = at % 128 != 0
            where[c, r] = (odd, 32 * sum(1 for w in where.values() if w[0] == odd), at // 128)

    def first_product(k, slot):
        for odd, at in ((False, 64), (True, 0)):
            rows = jnp.concatenate(
                [
                    jnp.concatenate(
                        [
                            wide_ref[w[2] + j, pl.ds(k, GROUP, stride=PITCH), :].astype(bf16)
                            for j in range(2)
                        ],
                        axis=1,
                    )
                    for w in where.values()
                    if w[0] == odd
                ],
                axis=0,
            )
            weights = wu_ref[k, at : at + 256, :]
            half = jnp.dot(rows, weights, preferred_element_type=f32).astype(bf16)
            for (c, r), w in where.items():
                if w[0] == odd:
                    half_ref[slot, c, 32 * r : 32 * r + 32, :] = half[w[1] : w[1] + 32]

    def second_product(k, slot, bloch_ref):
        for c in range(4):
            b_re, b_im = hermitian(*rotate(ut_ref[k], half_ref[slot, c]))
            bloch_ref[c, :, 0:128] = b_re.astype(bf16)
            bloch_ref[c, :, 128:256] = b_im.astype(bf16)

    sums = [jnp.zeros((1, 128), f32) for _ in range(9)]

    def currents(k, bloch_ref, flow_ref):
        for a in range(3):
            v = bloch_ref[1 + a]
            v_re, v_im = v[:, 0:128], v[:, 128:256]
            rhs = jnp.concatenate(
                [v, zero, jnp.concatenate([-v_im, v_re], axis=1), zero], axis=0
            )
            prod = jnp.dot(sb_ref[k], rhs, preferred_element_type=f32)
            p_re = prod[:, 0:128]
            p_im = prod[:, 128:256]
            flow_ref[a, :, 0:128] = p_re + flip_square(p_re)
            flow_ref[a, :, 128:256] = p_im - flip_square(p_im)

    def kubo(k, bloch_ref, flow_ref):
        diag = jnp.where(eye, bloch_ref[0, :, 0:128].astype(f32), 0.0)
        e_row = jnp.sum(diag, axis=0, keepdims=True)
        e_col = jnp.sum(diag, axis=1, keepdims=True)
        occupation = 1.0 / (1.0 + jnp.exp((e_row - fermi) / smearing))
        parts = [None] * 9
        for at in range(0, WF, 16):
            rows = slice(at, at + 16)
            gap = e_col[rows] - e_row
            weight = -1.0 / (gap * gap + broadening * broadening)
            v = [
                [bloch_ref[1 + b, rows, 128 * p : 128 * (p + 1)].astype(f32) for p in range(2)]
                for b in range(3)
            ]
            for a in range(3):
                c_re = flow_ref[a, rows, 0:128] * weight
                c_im = flow_ref[a, rows, 128:256] * weight
                for b in range(3):
                    term = c_re * v[b][1] - c_im * v[b][0]
                    ab = 3 * a + b
                    parts[ab] = term if parts[ab] is None else parts[ab] + term
        for ab in range(9):
            curve = jnp.sum(parts[ab], axis=0, keepdims=True)
            curve_ref[ab, k : k + 1, :] = curve[:, 0:WF]
            sums[ab] = sums[ab] + occupation * curve

    steps = QUARTER // PER_STEP
    for i in range(steps + 1):
        for q in range(PER_STEP):
            if i < steps:
                first_product(i * PER_STEP + q, i % 2 * PER_STEP + q)
        for q in range(PER_STEP):
            if i > 0:
                before = (i - 1) % 2 * PER_STEP + q
                currents((i - 1) * PER_STEP + q, bloch_refs[before], flow_refs[q])
                kubo((i - 1) * PER_STEP + q, bloch_refs[before], flow_refs[q])
            if i < steps:
                slot = i % 2 * PER_STEP + q
                second_product(i * PER_STEP + q, slot, bloch_refs[slot])

    lane8 = lax.broadcasted_iota(jnp.int32, (8, 128), 1)
    row8 = lax.broadcasted_iota(jnp.int32, (8, 128), 0)
    packed = jnp.zeros((8, 128), f32)
    for ab in range(8):
        packed = jnp.where(row8 == ab, sums[ab], packed)
    last = jnp.broadcast_to(sums[8], (8, 128))
    for t in range(3):
        moved = pltpu.roll(last, 96 - 32 * t, 1)
        packed = jnp.where((lane8 >= WF) & (row8 == t), moved, packed)
    total_ref[...] = jnp.broadcast_to(packed[None], total_ref.shape)


def bands(count, prepared, got, level):
    shapes = [(9, QUARTER, WF), (count, 8, 128)]
    vmem = pl.BlockSpec(memory_space=pltpu.VMEM)
    return pl.pallas_call(
        bands_kernel,
        in_specs=[vmem] * 5,
        out_specs=[vmem] * 2,
        out_shape=[jax.ShapeDtypeStruct(shape, f32) for shape in shapes],
        scratch_shapes=[
            pltpu.VMEM((KEPT // 128, GROUP * PITCH, 128), f32),
            pltpu.VMEM((2 * PER_STEP, 4, WF, 256), bf16),
        ]
        + [pltpu.VMEM((4, WF, 256), bf16)] * (2 * PER_STEP)
        + [pltpu.VMEM((3, WF, 256), f32)] * PER_STEP,
        compiler_params=pltpu.CompilerParams(vmem_limit_bytes=30 << 20),
        name="bands",
    )(*prepared, got, level)


def exchange(value, axes):
    return lax.all_to_all(value, axes, split_axis=0, concat_axis=0, tiled=True)


def on_device(hamiltonian, eigvecs, spin, k_indices, r_vectors, degeneracy, fermi_level):
    own = hamiltonian.shape[0]
    count = lax.axis_size("z") * lax.axis_size("y") * lax.axis_size("core") * lax.axis_size("x")
    pieces = pack(hamiltonian, k_indices.T, count)
    hopping = exchange(pieces, ALL)
    column = lax.axis_index("x").astype(jnp.int32).reshape(1)
    vectors = pltpu.with_memory_space_constraint(eigvecs, pltpu.HBM)
    *prepared, level = sides(column, vectors, spin, fermi_level.reshape(1, 1))
    layer = lax.axis_index("z")
    mine = lax.dynamic_slice(hopping, (layer * GROUP, 0, 0), (GROUP, own, WIDE))
    k_rows = mine.reshape(8, 4, own, WIDE)[:, 0, :, PIECE:]
    k_rows = k_rows.transpose(0, 2, 1).reshape(8 * (WIDE - PIECE), own).astype(f32)
    lattice = jnp.concatenate(
        [r_vectors.T.astype(f32), jnp.broadcast_to(degeneracy.astype(f32)[None], (5, NR))], axis=0
    )
    entries = interpolate(k_rows, lattice, hopping.reshape(NR, WIDE))
    entries, level, *prepared = lax.optimization_barrier((entries, level, *prepared))
    got = exchange(entries, PLANE)
    curvature, copies = bands(count, prepared, got, level)
    total_points = k_indices.shape[0] * count // 4
    total = jnp.sum(exchange(copies, ALL), axis=0) * (1.0 / math.sqrt(total_points))
    last = total[0:3, WF:].reshape(1, WF)
    totals = jnp.concatenate([total[:, :WF], last], axis=0)
    return (curvature.transpose(0, 2, 1), totals)


def solution(mesh):
    fine = Mesh(mesh.devices.reshape(4, 4, 2, 4), ALL)
    ka = ("z", "y", "core")
    in_specs = (P(ALL, None, None), P(ka, None, None, None), P(), P(ka, None), P(), P(), P())
    out_specs = (P(None, None, ALL), P())
    return jax.shard_map(
        on_device, mesh=fine, in_specs=in_specs, out_specs=out_specs, check_vma=False
    )
```

```python
import math

import jax
import jax.numpy as jnp
from jax import lax
from jax.experimental import pallas as pl
from jax.experimental.pallas import tpu as pltpu
from jax.sharding import Mesh, PartitionSpec as P

WF = 96
GRID = 64
NR = 1024
GROUP = 32
ROWS = 3
PIECE = ROWS * 2 * WF
WIDE = 640
KEPT = 4 * PIECE
QUARTER = 16
PITCH = 17
STEP_K = 128
PER_STEP = 4
SIDE_STEP = 4

broadening = 0.5
smearing = 0.1

ALL = ("z", "y", "core", "x")
PLANE = ("y", "core", "x")

f32 = jnp.float32
bf16 = jnp.bfloat16

SINE = (3.14159264, -5.16771009, 2.55007766, -0.59829216, 0.07765941)
COSINE = (0.99999995, -4.93479286, 4.05841192, -1.33188016, 0.2196968)


def whole(shape):
    return pl.BlockSpec(shape, lambda *_: (0,) * len(shape))


def horner(coefficients, q):
    value = coefficients[-1]
    for c in coefficients[-2::-1]:
        value = value * q + c
    return value


def turn(f):
    q = f * f
    s = f * horner(SINE, q)
    twice = s + s
    return 1.0 - twice * s, twice * horner(COSINE, q)


def flip(x):
    return jnp.transpose(x, (1, 0))


def flip_square(x):
    pad = jnp.zeros((32, 128), f32)
    return flip(jnp.concatenate([x, pad], axis=0))[0:WF]


def pack_kernel(ham_ref, k_ref, out_ref, piece_ref, points_ref, sems):
    lane = lax.broadcasted_iota(jnp.int32, (8, 128), 1)
    points_ref[...] = jnp.zeros_like(points_ref)
    points_ref[0:3, 64:128] = k_ref[...].astype(f32)
    points = points_ref[...]
    loaded = {}
    copies = []

    def tile(part, t):
        if (part, t) not in loaded:
            loaded[part, t] = ham_ref[:, part, 128 * t : 128 * (t + 1)].astype(f32)
        return loaded[part, t]

    def segment(part, line, start, size, at):
        first = WF * line + start
        shift = (at - first) % 128
        move = lambda t: pltpu.roll(tile(part, t), shift, 1) if shift else tile(part, t)
        value = move(first // 128)
        if (first + size - 1) // 128 != first // 128:
            cut = at + 128 - first % 128
            value = jnp.where(lane < cut, value, move(first // 128 + 1))
        return value

    layout = [
        ((0, 0, 0, 96, 0), (1, 0, 0, 32, 96)),
        ((1, 0, 32, 64, 0), (0, 1, 0, 64, 64)),
        ((0, 1, 64, 32, 0), (1, 1, 0, 96, 32)),
        ((0, 2, 0, 96, 0), (1, 2, 0, 32, 96)),
        ((1, 2, 32, 64, 0), None),
    ]
    for g in range(GROUP):
        for t, (left, right) in enumerate(layout):
            part, r, start, size, at = left
            value = segment(part, GROUP * r + g, start, size, at)
            if right is None:
                other = points
            else:
                other = segment(right[0], GROUP * right[1] + g, *right[2:])
            value = jnp.where(lane < size, value, other)
            piece_ref[g, :, 128 * t : 128 * (t + 1)] = value.astype(bf16)
        if g % 8 == 7:
            for z in range(out_ref.shape[0] // GROUP):
                copies.append(
                    pltpu.make_async_copy(
                        piece_ref.at[pl.ds(g - 7, 8)],
                        out_ref.at[pl.ds(GROUP * z + g - 7, 8)],
                        sems.at[g // 8, z],
                    )
                )
                copies[-1].start()
    for copy in copies:
        copy.wait()


def pack(hamiltonian, k_rows, count):
    own = hamiltonian.shape[0]
    vmem = pl.BlockSpec(memory_space=pltpu.VMEM)
    return pl.pallas_call(
        pack_kernel,
        in_specs=[vmem, vmem],
        out_specs=pl.BlockSpec(memory_space=pl.ANY),
        out_shape=jax.ShapeDtypeStruct((count, own, WIDE), bf16),
        scratch_shapes=[
            pltpu.VMEM((GROUP, own, WIDE), bf16),
            pltpu.VMEM((8, 128), f32),
            pltpu.SemaphoreType.DMA((4, count // GROUP)),
        ],
        name="pack",
    )(hamiltonian, k_rows)


def turn_hopping(hop_ref, w_ref):
    lane = lax.broadcasted_iota(jnp.int32, (NR, 128), 1)
    tiles = [hop_ref[:, 128 * t : 128 * (t + 1)].astype(f32) for t in range(5)]
    ups = [pltpu.roll(t, 96, 1) for t in tiles]
    downs = [pltpu.roll(t, 32, 1) for t in tiles]
    for t in range(5):
        up = jnp.where(lane < 96, ups[(t - 1) % 5], ups[t])
        down = jnp.where(lane < 32, downs[t], downs[(t + 1) % 5])
        place = (lane + 128 * t) % (2 * WF)
        turned = jnp.where(place < WF, -down, up)
        w_ref[:, 128 * t : 128 * (t + 1)] = turned.astype(bf16)


def phase_block(k, lat_ref, p_ref):
    r = [lat_ref[a : a + 1, :] for a in range(3)]
    inverse = 1.0 / lat_ref[3:4, :]
    turns = jnp.dot(
        k.astype(bf16), (lat_ref[...] * (1.0 / GRID)).astype(bf16), preferred_element_type=f32
    )
    cosine, sine = turn(turns - jnp.floor(turns + 0.5))
    for c in range(4):
        rows = slice(c * STEP_K, (c + 1) * STEP_K)
        if c == 0:
            re, im = cosine * inverse, sine * inverse
        else:
            coord = r[c - 1] * inverse
            re, im = sine * (-coord), cosine * coord
        p_ref[rows, 0:NR] = re.astype(bf16)
        p_ref[rows, NR : 2 * NR] = im.astype(bf16)


def interpolate_kernel(k_ref, lat_ref, hop_ref, out_ref, w_ref, *p_refs):
    steps = GROUP * QUARTER // STEP_K
    per = STEP_K // QUARTER
    lane = lax.broadcasted_iota(jnp.int32, (STEP_K, 128), 1)

    def phases(i):
        phase_block(k_ref[i * STEP_K : (i + 1) * STEP_K, :], lat_ref, p_refs[i % 2])

    phases(0)
    turn_hopping(hop_ref, w_ref)
    for i in range(steps):
        if i + 1 < steps:
            phases(i + 1)
        p_ref = p_refs[i % 2]
        summed = jnp.dot(p_ref[:, 0:NR], hop_ref[...], preferred_element_type=f32)
        summed += jnp.dot(p_ref[:, NR : 2 * NR], w_ref[...], preferred_element_type=f32)
        for pair in range(2):
            even = summed[2 * pair * STEP_K : (2 * pair + 1) * STEP_K]
            odd = summed[(2 * pair + 1) * STEP_K : (2 * pair + 2) * STEP_K]
            shifted = [pltpu.roll(odd[:, 128 * t : 128 * (t + 1)], 64, 1) for t in range(5)]
            for t in range(9):
                if t < 4:
                    tile = even[:, 128 * t : 128 * (t + 1)]
                elif t == 4:
                    tile = jnp.where(lane < 64, even[:, 512:640], shifted[0])
                else:
                    tile = jnp.where(lane < 64, shifted[t - 5], shifted[t - 4])
                at = pair * 2 * PIECE + 128 * t
                value = tile.reshape(per, QUARTER, 128).astype(bf16)
                out_ref[i * per : (i + 1) * per, :, at : at + 128] = value


def interpolate(k_rows, lattice, hopping):
    vmem = pl.BlockSpec(memory_space=pltpu.VMEM)
    return pl.pallas_call(
        interpolate_kernel,
        in_specs=[vmem, vmem, vmem],
        out_specs=vmem,
        out_shape=jax.ShapeDtypeStruct((GROUP, QUARTER, KEPT), bf16),
        scratch_shapes=[
            pltpu.VMEM((NR, WIDE), bf16),
            pltpu.VMEM((4 * STEP_K, 2 * NR), bf16),
            pltpu.VMEM((4 * STEP_K, 2 * NR), bf16),
        ],
        compiler_params=pltpu.CompilerParams(vmem_limit_bytes=30 << 20),
        name="interpolate",
    )(k_rows, lattice, hopping)


def rotate(ut, half):
    h_re, h_im = half[:, 0:128], half[:, 128:256]
    zero = jnp.zeros((32, 256), bf16)
    rhs = jnp.concatenate(
        [half, zero, jnp.concatenate([h_im, -h_re], axis=1), zero], axis=0
    )
    full = jnp.dot(ut, rhs, preferred_element_type=f32)
    return full[:, 0:128], full[:, 128:256]


def hermitian(re, im):
    return (re + flip_square(re)) * 0.5, (im - flip_square(im)) * 0.5


def sides_kernel(column_ref, vec_ref, spin_ref, fermi_ref, wu_ref, ut_ref, sb_ref, level_ref, sp_ref):
    @pl.when(pl.program_id(0) == 0)
    def _():
        level_ref[...] = jnp.full(level_ref.shape, fermi_ref[0, 0], f32)
        sp_ref[...] = jnp.zeros_like(sp_ref)
        spin_re = spin_ref[0].astype(f32)
        spin_im = spin_ref[1].astype(f32)
        sp_ref[:, 0:WF] = ((spin_re + flip(spin_re)) * 0.5).astype(bf16)
        sp_ref[:, WF : 2 * WF] = ((spin_im - flip(spin_im)) * 0.5).astype(bf16)

    wu_ref[...] = jnp.zeros_like(wu_ref)
    ut_ref[...] = jnp.zeros_like(ut_ref)
    for q in range(SIDE_STEP):
        u_re = vec_ref[q, 0]
        u_im = vec_ref[q, 1]
        wu_ref[q, 64 : 64 + WF, 0:WF] = u_re
        wu_ref[q, 64 : 64 + WF, 128 : 128 + WF] = u_im
        wu_ref[q, 160 : 160 + WF, 0:WF] = -u_im
        wu_ref[q, 160 : 160 + WF, 128 : 128 + WF] = u_re
        ut_ref[q, :, 0:WF] = flip(u_re.astype(f32)).astype(bf16)
        ut_ref[q, :, 128 : 128 + WF] = flip(u_im.astype(f32)).astype(bf16)
    for q in range(SIDE_STEP):
        half = jnp.dot(sp_ref[...], wu_ref[q, 64:320, :], preferred_element_type=f32)
        s_re, s_im = hermitian(*rotate(ut_ref[q], half.astype(bf16)))
        sb_ref[q, :, 0:128] = s_re.astype(bf16)
        sb_ref[q, :, 128:256] = s_im.astype(bf16)


def sides(column, vectors, spin, fermi):
    per = QUARTER // SIDE_STEP
    shapes = [(320, 256), (WF, 256), (WF, 256)]
    grid_spec = pltpu.PrefetchScalarGridSpec(
        num_scalar_prefetch=1,
        grid=(per,),
        in_specs=[
            pl.BlockSpec((SIDE_STEP, 2, WF, WF), lambda i, c: (c[0] * per + i, 0, 0, 0)),
            whole((2, WF, WF)),
            pl.BlockSpec(memory_space=pltpu.SMEM),
        ],
        out_specs=[pl.BlockSpec((SIDE_STEP, *s), lambda i, c: (i, 0, 0)) for s in shapes]
        + [whole((8, 128))],
        scratch_shapes=[pltpu.VMEM((WF, 256), bf16)],
    )
    return pl.pallas_call(
        sides_kernel,
        grid_spec=grid_spec,
        out_shape=[jax.ShapeDtypeStruct((QUARTER, *s), bf16) for s in shapes]
        + [jax.ShapeDtypeStruct((8, 128), f32)],
        compiler_params=pltpu.CompilerParams(
            dimension_semantics=("arbitrary",), vmem_limit_bytes=30 << 20
        ),
        cost_estimate=pl.CostEstimate(
            flops=QUARTER * 4 * 256 * 256 * 256,
            transcendentals=0,
            bytes_accessed=QUARTER * 2 * 256 * (320 + 4 * WF),
        ),
        name="sides",
    )(column, vectors, spin, fermi)


def bands_kernel(
    wu_ref, ut_ref, sb_ref, got_ref, level_ref, curve_ref, total_ref,
    wide_ref, half_ref, *others,
):
    bloch_refs, flow_refs = others[: 2 * PER_STEP], others[2 * PER_STEP :]
    for t in range(KEPT // 128):
        tile = got_ref[:, :, 128 * t : 128 * (t + 1)].astype(f32)
        for s in range(GROUP):
            wide_ref[t, PITCH * s : PITCH * s + QUARTER, :] = tile[s]

    lane = lax.broadcasted_iota(jnp.int32, (WF, 128), 1)
    row = lax.broadcasted_iota(jnp.int32, (WF, 128), 0)
    eye = lane == row
    fermi = level_ref[0:1, :]
    zero = jnp.zeros((32, 256), bf16)

    where = {}
    for c in range(4):
        for r in range(ROWS):
            at = c * PIECE + r * 2 * WF
            odd = at % 128 != 0
            where[c, r] = (odd, 32 * sum(1 for w in where.values() if w[0] == odd), at // 128)

    def first_product(k, slot):
        for odd, at in ((False, 64), (True, 0)):
            rows = jnp.concatenate(
                [
                    jnp.concatenate(
                        [
                            wide_ref[w[2] + j, pl.ds(k, GROUP, stride=PITCH), :].astype(bf16)
                            for j in range(2)
                        ],
                        axis=1,
                    )
                    for w in where.values()
                    if w[0] == odd
                ],
                axis=0,
            )
            weights = wu_ref[k, at : at + 256, :]
            half = jnp.dot(rows, weights, preferred_element_type=f32).astype(bf16)
            for (c, r), w in where.items():
                if w[0] == odd:
                    half_ref[slot, c, 32 * r : 32 * r + 32, :] = half[w[1] : w[1] + 32]

    def second_product(k, slot, bloch_ref):
        for c in range(4):
            b_re, b_im = hermitian(*rotate(ut_ref[k], half_ref[slot, c]))
            bloch_ref[c, :, 0:128] = b_re.astype(bf16)
            bloch_ref[c, :, 128:256] = b_im.astype(bf16)

    sums = [jnp.zeros((1, 128), f32) for _ in range(9)]

    def currents(k, bloch_ref, flow_ref):
        for a in range(3):
            v = bloch_ref[1 + a]
            v_re, v_im = v[:, 0:128], v[:, 128:256]
            rhs = jnp.concatenate(
                [v, zero, jnp.concatenate([-v_im, v_re], axis=1), zero], axis=0
            )
            prod = jnp.dot(sb_ref[k], rhs, preferred_element_type=f32)
            p_re = prod[:, 0:128]
            p_im = prod[:, 128:256]
            flow_ref[a, :, 0:128] = p_re + flip_square(p_re)
            flow_ref[a, :, 128:256] = p_im - flip_square(p_im)

    def kubo(k, bloch_ref, flow_ref):
        diag = jnp.where(eye, bloch_ref[0, :, 0:128].astype(f32), 0.0)
        e_row = jnp.sum(diag, axis=0, keepdims=True)
        e_col = jnp.sum(diag, axis=1, keepdims=True)
        occupation = 1.0 / (1.0 + jnp.exp((e_row - fermi) / smearing))
        parts = [None] * 9
        for at in range(0, WF, 16):
            rows = slice(at, at + 16)
            gap = e_col[rows] - e_row
            weight = -1.0 / (gap * gap + broadening * broadening)
            v = [
                [bloch_ref[1 + b, rows, 128 * p : 128 * (p + 1)].astype(f32) for p in range(2)]
                for b in range(3)
            ]
            for a in range(3):
                c_re = flow_ref[a, rows, 0:128] * weight
                c_im = flow_ref[a, rows, 128:256] * weight
                for b in range(3):
                    term = c_re * v[b][1] - c_im * v[b][0]
                    ab = 3 * a + b
                    parts[ab] = term if parts[ab] is None else parts[ab] + term
        for ab in range(9):
            curve = jnp.sum(parts[ab], axis=0, keepdims=True)
            curve_ref[ab, k : k + 1, :] = curve[:, 0:WF]
            sums[ab] = sums[ab] + occupation * curve

    steps = QUARTER // PER_STEP
    for i in range(steps + 1):
        for q in range(PER_STEP):
            if i < steps:
                first_product(i * PER_STEP + q, i % 2 * PER_STEP + q)
        for q in range(PER_STEP):
            if i > 0:
                before = (i - 1) % 2 * PER_STEP + q
                currents((i - 1) * PER_STEP + q, bloch_refs[before], flow_refs[q])
                kubo((i - 1) * PER_STEP + q, bloch_refs[before], flow_refs[q])
            if i < steps:
                slot = i % 2 * PER_STEP + q
                second_product(i * PER_STEP + q, slot, bloch_refs[slot])

    lane8 = lax.broadcasted_iota(jnp.int32, (8, 128), 1)
    row8 = lax.broadcasted_iota(jnp.int32, (8, 128), 0)
    packed = jnp.zeros((8, 128), f32)
    for ab in range(8):
        packed = jnp.where(row8 == ab, sums[ab], packed)
    last = jnp.broadcast_to(sums[8], (8, 128))
    for t in range(3):
        moved = pltpu.roll(last, 96 - 32 * t, 1)
        packed = jnp.where((lane8 >= WF) & (row8 == t), moved, packed)
    total_ref[...] = jnp.broadcast_to(packed[None], total_ref.shape)


def bands(count, prepared, got, level):
    shapes = [(9, QUARTER, WF), (count, 8, 128)]
    vmem = pl.BlockSpec(memory_space=pltpu.VMEM)
    return pl.pallas_call(
        bands_kernel,
        in_specs=[vmem] * 5,
        out_specs=[vmem] * 2,
        out_shape=[jax.ShapeDtypeStruct(shape, f32) for shape in shapes],
        scratch_shapes=[
            pltpu.VMEM((KEPT // 128, GROUP * PITCH, 128), f32),
            pltpu.VMEM((2 * PER_STEP, 4, WF, 256), bf16),
        ]
        + [pltpu.VMEM((4, WF, 256), bf16)] * (2 * PER_STEP)
        + [pltpu.VMEM((3, WF, 256), f32)] * PER_STEP,
        compiler_params=pltpu.CompilerParams(vmem_limit_bytes=30 << 20),
        name="bands",
    )(*prepared, got, level)


def total_sums(parts, scale):
    def kernel(parts_ref, out_ref):
        total = jnp.sum(parts_ref[...], axis=0) * scale
        out_ref[0:8, :] = total[:, 0:WF]
        lane = lax.broadcasted_iota(jnp.int32, (8, 128), 1)
        row = lax.broadcasted_iota(jnp.int32, (8, 128), 0)
        last = jnp.zeros((8, 128), f32)
        for t in range(3):
            moved = pltpu.roll(total, 32 + 32 * t, 1)
            keep = (row == t) & (lane >= 32 * t) & (lane < 32 * (t + 1))
            last = jnp.where(keep, moved, last)
        out_ref[8:9, :] = jnp.sum(last, axis=0, keepdims=True)[:, 0:WF]

    vmem = pl.BlockSpec(memory_space=pltpu.VMEM)
    return pl.pallas_call(
        kernel,
        in_specs=[vmem],
        out_specs=vmem,
        out_shape=jax.ShapeDtypeStruct((9, WF), f32),
        name="total_sums",
    )(parts)


def exchange(value, axes):
    return lax.all_to_all(value, axes, split_axis=0, concat_axis=0, tiled=True)


def on_device(hamiltonian, eigvecs, spin, k_indices, r_vectors, degeneracy, fermi_level):
    own = hamiltonian.shape[0]
    count = lax.axis_size("z") * lax.axis_size("y") * lax.axis_size("core") * lax.axis_size("x")
    pieces = pack(hamiltonian, k_indices.T, count)
    hopping = exchange(pieces, ALL)
    column = lax.axis_index("x").astype(jnp.int32).reshape(1)
    vectors = pltpu.with_memory_space_constraint(eigvecs, pltpu.HBM)
    *prepared, level = sides(column, vectors, spin, fermi_level.reshape(1, 1))
    layer = lax.axis_index("z")
    mine = lax.dynamic_slice(hopping, (layer * GROUP, 0, 0), (GROUP, own, WIDE))
    k_rows = mine.reshape(8, 4, own, WIDE)[:, 0, :, PIECE:]
    k_rows = k_rows.transpose(0, 2, 1).reshape(8 * (WIDE - PIECE), own).astype(f32)
    lattice = jnp.concatenate(
        [r_vectors.T.astype(f32), jnp.broadcast_to(degeneracy.astype(f32)[None], (5, NR))], axis=0
    )
    entries = interpolate(k_rows, lattice, hopping.reshape(NR, WIDE))
    entries, level, *prepared = lax.optimization_barrier((entries, level, *prepared))
    got = exchange(entries, PLANE)
    curvature, copies = bands(count, prepared, got, level)
    total_points = k_indices.shape[0] * count // 4
    totals = total_sums(exchange(copies, ALL), 1.0 / math.sqrt(total_points))
    return (curvature.transpose(0, 2, 1), totals)


def solution(mesh):
    fine = Mesh(mesh.devices.reshape(4, 4, 2, 4), ALL)
    ka = ("z", "y", "core")
    in_specs = (P(ALL, None, None), P(ka, None, None, None), P(), P(ka, None), P(), P(), P())
    out_specs = (P(None, None, ALL), P())
    return jax.shard_map(
        on_device, mesh=fine, in_specs=in_specs, out_specs=out_specs, check_vma=False
    )
```

```python
import math

import jax
import jax.numpy as jnp
from jax import lax
from jax.experimental import pallas as pl
from jax.experimental.pallas import tpu as pltpu
from jax.sharding import Mesh, PartitionSpec as P

WF = 96
GRID = 64
NR = 1024
GROUP = 32
ROWS = 3
PIECE = ROWS * 2 * WF
WIDE = 640
KEPT = 4 * PIECE
QUARTER = 16
PITCH = 17
STEP_K = 128
PER_STEP = 4
SIDE_STEP = 4

broadening = 0.5
smearing = 0.1

ALL = ("z", "y", "core", "x")
PLANE = ("y", "core", "x")

f32 = jnp.float32
bf16 = jnp.bfloat16

SINE = (3.14159264, -5.16771009, 2.55007766, -0.59829216, 0.07765941)
COSINE = (0.99999995, -4.93479286, 4.05841192, -1.33188016, 0.2196968)


def whole(shape):
    return pl.BlockSpec(shape, lambda *_: (0,) * len(shape))


def horner(coefficients, q):
    value = coefficients[-1]
    for c in coefficients[-2::-1]:
        value = value * q + c
    return value


def turn(f):
    q = f * f
    s = f * horner(SINE, q)
    twice = s + s
    return 1.0 - twice * s, twice * horner(COSINE, q)


def flip(x):
    return jnp.transpose(x, (1, 0))


def flip_square(x):
    pad = jnp.zeros((32, 128), f32)
    return flip(jnp.concatenate([x, pad], axis=0))[0:WF]


def pack_kernel(ham_ref, k_ref, out_ref, piece_ref, points_ref, sems):
    lane = lax.broadcasted_iota(jnp.int32, (8, 128), 1)
    points_ref[...] = jnp.zeros_like(points_ref)
    points_ref[0:3, 64:128] = k_ref[...].astype(f32)
    points = points_ref[...]
    loaded = {}
    copies = []

    def tile(part, t):
        if (part, t) not in loaded:
            loaded[part, t] = ham_ref[:, part, 128 * t : 128 * (t + 1)].astype(f32)
        return loaded[part, t]

    def segment(part, line, start, size, at):
        first = WF * line + start
        shift = (at - first) % 128
        move = lambda t: pltpu.roll(tile(part, t), shift, 1) if shift else tile(part, t)
        value = move(first // 128)
        if (first + size - 1) // 128 != first // 128:
            cut = at + 128 - first % 128
            value = jnp.where(lane < cut, value, move(first // 128 + 1))
        return value

    layout = [
        ((0, 0, 0, 96, 0), (1, 0, 0, 32, 96)),
        ((1, 0, 32, 64, 0), (0, 1, 0, 64, 64)),
        ((0, 1, 64, 32, 0), (1, 1, 0, 96, 32)),
        ((0, 2, 0, 96, 0), (1, 2, 0, 32, 96)),
        ((1, 2, 32, 64, 0), None),
    ]
    for g in range(GROUP):
        for t, (left, right) in enumerate(layout):
            part, r, start, size, at = left
            value = segment(part, GROUP * r + g, start, size, at)
            if right is None:
                other = points
            else:
                other = segment(right[0], GROUP * right[1] + g, *right[2:])
            value = jnp.where(lane < size, value, other)
            piece_ref[g, :, 128 * t : 128 * (t + 1)] = value.astype(bf16)
        if g % 8 == 7:
            for z in range(out_ref.shape[0] // GROUP):
                copies.append(
                    pltpu.make_async_copy(
                        piece_ref.at[pl.ds(g - 7, 8)],
                        out_ref.at[pl.ds(GROUP * z + g - 7, 8)],
                        sems.at[g // 8, z],
                    )
                )
                copies[-1].start()
    for copy in copies:
        copy.wait()


def pack(hamiltonian, k_rows, count):
    own = hamiltonian.shape[0]
    vmem = pl.BlockSpec(memory_space=pltpu.VMEM)
    return pl.pallas_call(
        pack_kernel,
        in_specs=[vmem, vmem],
        out_specs=pl.BlockSpec(memory_space=pl.ANY),
        out_shape=jax.ShapeDtypeStruct((count, own, WIDE), bf16),
        scratch_shapes=[
            pltpu.VMEM((GROUP, own, WIDE), bf16),
            pltpu.VMEM((8, 128), f32),
            pltpu.SemaphoreType.DMA((4, count // GROUP)),
        ],
        name="pack",
    )(hamiltonian, k_rows)


def turn_hopping(hop_ref, w_ref):
    lane = lax.broadcasted_iota(jnp.int32, (NR, 128), 1)
    tiles = [hop_ref[:, 128 * t : 128 * (t + 1)].astype(f32) for t in range(5)]
    ups = [pltpu.roll(t, 96, 1) for t in tiles]
    downs = [pltpu.roll(t, 32, 1) for t in tiles]
    for t in range(5):
        up = jnp.where(lane < 96, ups[(t - 1) % 5], ups[t])
        down = jnp.where(lane < 32, downs[t], downs[(t + 1) % 5])
        place = (lane + 128 * t) % (2 * WF)
        turned = jnp.where(place < WF, -down, up)
        w_ref[:, 128 * t : 128 * (t + 1)] = turned.astype(bf16)


def phase_block(k, lat_ref, p_ref):
    r = [lat_ref[a : a + 1, :] for a in range(3)]
    inverse = 1.0 / lat_ref[3:4, :]
    turns = jnp.dot(
        k.astype(bf16), (lat_ref[...] * (1.0 / GRID)).astype(bf16), preferred_element_type=f32
    )
    cosine, sine = turn(turns - jnp.floor(turns + 0.5))
    for c in range(4):
        rows = slice(c * STEP_K, (c + 1) * STEP_K)
        if c == 0:
            re, im = cosine * inverse, sine * inverse
        else:
            coord = r[c - 1] * inverse
            re, im = sine * (-coord), cosine * coord
        p_ref[rows, 0:NR] = re.astype(bf16)
        p_ref[rows, NR : 2 * NR] = im.astype(bf16)


def interpolate_kernel(k_ref, lat_ref, hop_ref, out_ref, w_ref, *p_refs):
    steps = GROUP * QUARTER // STEP_K
    per = STEP_K // QUARTER
    lane = lax.broadcasted_iota(jnp.int32, (STEP_K, 128), 1)

    def phases(i):
        phase_block(k_ref[i * STEP_K : (i + 1) * STEP_K, :], lat_ref, p_refs[i % 2])

    phases(0)
    for i in range(steps):
        p_ref = p_refs[i % 2]
        summed = jnp.dot(p_ref[:, 0:NR], hop_ref[...], preferred_element_type=f32)
        if i == 0:
            turn_hopping(hop_ref, w_ref)
        if i + 1 < steps:
            phases(i + 1)
        summed += jnp.dot(p_ref[:, NR : 2 * NR], w_ref[...], preferred_element_type=f32)
        for pair in range(2):
            even = summed[2 * pair * STEP_K : (2 * pair + 1) * STEP_K]
            odd = summed[(2 * pair + 1) * STEP_K : (2 * pair + 2) * STEP_K]
            shifted = [pltpu.roll(odd[:, 128 * t : 128 * (t + 1)], 64, 1) for t in range(5)]
            for t in range(9):
                if t < 4:
                    tile = even[:, 128 * t : 128 * (t + 1)]
                elif t == 4:
                    tile = jnp.where(lane < 64, even[:, 512:640], shifted[0])
                else:
                    tile = jnp.where(lane < 64, shifted[t - 5], shifted[t - 4])
                at = pair * 2 * PIECE + 128 * t
                value = tile.reshape(per, QUARTER, 128).astype(bf16)
                out_ref[i * per : (i + 1) * per, :, at : at + 128] = value


def interpolate(k_rows, lattice, hopping):
    vmem = pl.BlockSpec(memory_space=pltpu.VMEM)
    return pl.pallas_call(
        interpolate_kernel,
        in_specs=[vmem, vmem, vmem],
        out_specs=vmem,
        out_shape=jax.ShapeDtypeStruct((GROUP, QUARTER, KEPT), bf16),
        scratch_shapes=[
            pltpu.VMEM((NR, WIDE), bf16),
            pltpu.VMEM((4 * STEP_K, 2 * NR), bf16),
            pltpu.VMEM((4 * STEP_K, 2 * NR), bf16),
        ],
        compiler_params=pltpu.CompilerParams(vmem_limit_bytes=30 << 20),
        name="interpolate",
    )(k_rows, lattice, hopping)


def rotate(ut, half):
    h_re, h_im = half[:, 0:128], half[:, 128:256]
    zero = jnp.zeros((32, 256), bf16)
    rhs = jnp.concatenate(
        [half, zero, jnp.concatenate([h_im, -h_re], axis=1), zero], axis=0
    )
    full = jnp.dot(ut, rhs, preferred_element_type=f32)
    return full[:, 0:128], full[:, 128:256]


def hermitian(re, im):
    return (re + flip_square(re)) * 0.5, (im - flip_square(im)) * 0.5


def sides_kernel(column_ref, vec_ref, spin_ref, fermi_ref, wu_ref, ut_ref, sb_ref, level_ref, sp_ref):
    @pl.when(pl.program_id(0) == 0)
    def _():
        level_ref[...] = jnp.full(level_ref.shape, fermi_ref[0, 0], f32)
        sp_ref[...] = jnp.zeros_like(sp_ref)
        spin_re = spin_ref[0].astype(f32)
        spin_im = spin_ref[1].astype(f32)
        sp_ref[:, 0:WF] = ((spin_re + flip(spin_re)) * 0.5).astype(bf16)
        sp_ref[:, WF : 2 * WF] = ((spin_im - flip(spin_im)) * 0.5).astype(bf16)

    wu_ref[...] = jnp.zeros_like(wu_ref)
    ut_ref[...] = jnp.zeros_like(ut_ref)
    for q in range(SIDE_STEP):
        u_re = vec_ref[q, 0]
        u_im = vec_ref[q, 1]
        wu_ref[q, 64 : 64 + WF, 0:WF] = u_re
        wu_ref[q, 64 : 64 + WF, 128 : 128 + WF] = u_im
        wu_ref[q, 160 : 160 + WF, 0:WF] = -u_im
        wu_ref[q, 160 : 160 + WF, 128 : 128 + WF] = u_re
        ut_ref[q, :, 0:WF] = flip(u_re.astype(f32)).astype(bf16)
        ut_ref[q, :, 128 : 128 + WF] = flip(u_im.astype(f32)).astype(bf16)
    for q in range(SIDE_STEP):
        half = jnp.dot(sp_ref[...], wu_ref[q, 64:320, :], preferred_element_type=f32)
        s_re, s_im = hermitian(*rotate(ut_ref[q], half.astype(bf16)))
        sb_ref[q, :, 0:128] = s_re.astype(bf16)
        sb_ref[q, :, 128:256] = s_im.astype(bf16)


def sides(column, vectors, spin, fermi):
    per = QUARTER // SIDE_STEP
    shapes = [(320, 256), (WF, 256), (WF, 256)]
    grid_spec = pltpu.PrefetchScalarGridSpec(
        num_scalar_prefetch=1,
        grid=(per,),
        in_specs=[
            pl.BlockSpec((SIDE_STEP, 2, WF, WF), lambda i, c: (c[0] * per + i, 0, 0, 0)),
            whole((2, WF, WF)),
            pl.BlockSpec(memory_space=pltpu.SMEM),
        ],
        out_specs=[pl.BlockSpec((SIDE_STEP, *s), lambda i, c: (i, 0, 0)) for s in shapes]
        + [whole((8, 128))],
        scratch_shapes=[pltpu.VMEM((WF, 256), bf16)],
    )
    return pl.pallas_call(
        sides_kernel,
        grid_spec=grid_spec,
        out_shape=[jax.ShapeDtypeStruct((QUARTER, *s), bf16) for s in shapes]
        + [jax.ShapeDtypeStruct((8, 128), f32)],
        compiler_params=pltpu.CompilerParams(
            dimension_semantics=("arbitrary",), vmem_limit_bytes=30 << 20
        ),
        cost_estimate=pl.CostEstimate(
            flops=QUARTER * 4 * 256 * 256 * 256,
            transcendentals=0,
            bytes_accessed=QUARTER * 2 * 256 * (320 + 4 * WF),
        ),
        name="sides",
    )(column, vectors, spin, fermi)


def bands_kernel(
    wu_ref, ut_ref, sb_ref, got_ref, level_ref, curve_ref, total_ref,
    wide_ref, half_ref, *others,
):
    bloch_refs, flow_refs = others[: 2 * PER_STEP], others[2 * PER_STEP :]
    for t in range(KEPT // 128):
        tile = got_ref[:, :, 128 * t : 128 * (t + 1)].astype(f32)
        for s in range(GROUP):
            wide_ref[t, PITCH * s : PITCH * s + QUARTER, :] = tile[s]

    lane = lax.broadcasted_iota(jnp.int32, (WF, 128), 1)
    row = lax.broadcasted_iota(jnp.int32, (WF, 128), 0)
    eye = lane == row
    fermi = level_ref[0:1, :]
    zero = jnp.zeros((32, 256), bf16)

    where = {}
    for c in range(4):
        for r in range(ROWS):
            at = c * PIECE + r * 2 * WF
            odd = at % 128 != 0
            where[c, r] = (odd, 32 * sum(1 for w in where.values() if w[0] == odd), at // 128)

    def first_product(k, slot):
        for odd, at in ((False, 64), (True, 0)):
            rows = jnp.concatenate(
                [
                    jnp.concatenate(
                        [
                            wide_ref[w[2] + j, pl.ds(k, GROUP, stride=PITCH), :].astype(bf16)
                            for j in range(2)
                        ],
                        axis=1,
                    )
                    for w in where.values()
                    if w[0] == odd
                ],
                axis=0,
            )
            weights = wu_ref[k, at : at + 256, :]
            half = jnp.dot(rows, weights, preferred_element_type=f32).astype(bf16)
            for (c, r), w in where.items():
                if w[0] == odd:
                    half_ref[slot, c, 32 * r : 32 * r + 32, :] = half[w[1] : w[1] + 32]

    def second_product(k, slot, bloch_ref):
        for c in range(4):
            b_re, b_im = hermitian(*rotate(ut_ref[k], half_ref[slot, c]))
            bloch_ref[c, :, 0:128] = b_re.astype(bf16)
            bloch_ref[c, :, 128:256] = b_im.astype(bf16)

    sums = [jnp.zeros((1, 128), f32) for _ in range(9)]

    def currents(k, bloch_ref, flow_ref):
        for a in range(3):
            v = bloch_ref[1 + a]
            v_re, v_im = v[:, 0:128], v[:, 128:256]
            rhs = jnp.concatenate(
                [v, zero, jnp.concatenate([-v_im, v_re], axis=1), zero], axis=0
            )
            prod = jnp.dot(sb_ref[k], rhs, preferred_element_type=f32)
            p_re = prod[:, 0:128]
            p_im = prod[:, 128:256]
            flow_ref[a, :, 0:128] = p_re + flip_square(p_re)
            flow_ref[a, :, 128:256] = p_im - flip_square(p_im)

    def kubo(k, bloch_ref, flow_ref):
        diag = jnp.where(eye, bloch_ref[0, :, 0:128].astype(f32), 0.0)
        e_row = jnp.sum(diag, axis=0, keepdims=True)
        e_col = jnp.sum(diag, axis=1, keepdims=True)
        occupation = 1.0 / (1.0 + jnp.exp((e_row - fermi) / smearing))
        parts = [None] * 9
        for at in range(0, WF, 16):
            rows = slice(at, at + 16)
            gap = e_col[rows] - e_row
            weight = -1.0 / (gap * gap + broadening * broadening)
            v = [
                [bloch_ref[1 + b, rows, 128 * p : 128 * (p + 1)].astype(f32) for p in range(2)]
                for b in range(3)
            ]
            for a in range(3):
                c_re = flow_ref[a, rows, 0:128] * weight
                c_im = flow_ref[a, rows, 128:256] * weight
                for b in range(3):
                    term = c_re * v[b][1] - c_im * v[b][0]
                    ab = 3 * a + b
                    parts[ab] = term if parts[ab] is None else parts[ab] + term
        for ab in range(9):
            curve = jnp.sum(parts[ab], axis=0, keepdims=True)
            curve_ref[ab, k : k + 1, :] = curve[:, 0:WF]
            sums[ab] = sums[ab] + occupation * curve

    steps = QUARTER // PER_STEP
    for i in range(steps + 1):
        for q in range(PER_STEP):
            if i < steps:
                first_product(i * PER_STEP + q, i % 2 * PER_STEP + q)
        for q in range(PER_STEP):
            if i > 0:
                before = (i - 1) % 2 * PER_STEP + q
                currents((i - 1) * PER_STEP + q, bloch_refs[before], flow_refs[q])
                kubo((i - 1) * PER_STEP + q, bloch_refs[before], flow_refs[q])
            if i < steps:
                slot = i % 2 * PER_STEP + q
                second_product(i * PER_STEP + q, slot, bloch_refs[slot])

    lane8 = lax.broadcasted_iota(jnp.int32, (8, 128), 1)
    row8 = lax.broadcasted_iota(jnp.int32, (8, 128), 0)
    packed = jnp.zeros((8, 128), f32)
    for ab in range(8):
        packed = jnp.where(row8 == ab, sums[ab], packed)
    last = jnp.broadcast_to(sums[8], (8, 128))
    for t in range(3):
        moved = pltpu.roll(last, 96 - 32 * t, 1)
        packed = jnp.where((lane8 >= WF) & (row8 == t), moved, packed)
    total_ref[...] = jnp.broadcast_to(packed[None], total_ref.shape)


def bands(count, prepared, got, level):
    shapes = [(9, QUARTER, WF), (count, 8, 128)]
    vmem = pl.BlockSpec(memory_space=pltpu.VMEM)
    return pl.pallas_call(
        bands_kernel,
        in_specs=[vmem] * 5,
        out_specs=[vmem] * 2,
        out_shape=[jax.ShapeDtypeStruct(shape, f32) for shape in shapes],
        scratch_shapes=[
            pltpu.VMEM((KEPT // 128, GROUP * PITCH, 128), f32),
            pltpu.VMEM((2 * PER_STEP, 4, WF, 256), bf16),
        ]
        + [pltpu.VMEM((4, WF, 256), bf16)] * (2 * PER_STEP)
        + [pltpu.VMEM((3, WF, 256), f32)] * PER_STEP,
        compiler_params=pltpu.CompilerParams(vmem_limit_bytes=30 << 20),
        name="bands",
    )(*prepared, got, level)


def exchange(value, axes):
    return lax.all_to_all(value, axes, split_axis=0, concat_axis=0, tiled=True)


def on_device(hamiltonian, eigvecs, spin, k_indices, r_vectors, degeneracy, fermi_level):
    own = hamiltonian.shape[0]
    count = lax.axis_size("z") * lax.axis_size("y") * lax.axis_size("core") * lax.axis_size("x")
    pieces = pack(hamiltonian, k_indices.T, count)
    hopping = exchange(pieces, ALL)
    column = lax.axis_index("x").astype(jnp.int32).reshape(1)
    vectors = pltpu.with_memory_space_constraint(eigvecs, pltpu.HBM)
    *prepared, level = sides(column, vectors, spin, fermi_level.reshape(1, 1))
    layer = lax.axis_index("z")
    mine = lax.dynamic_slice(hopping, (layer * GROUP, 0, 0), (GROUP, own, WIDE))
    k_rows = mine.reshape(8, 4, own, WIDE)[:, 0, :, PIECE:]
    k_rows = k_rows.transpose(0, 2, 1).reshape(8 * (WIDE - PIECE), own).astype(f32)
    lattice = jnp.concatenate(
        [r_vectors.T.astype(f32), jnp.broadcast_to(degeneracy.astype(f32)[None], (5, NR))], axis=0
    )
    entries = interpolate(k_rows, lattice, hopping.reshape(NR, WIDE))
    entries, level, *prepared = lax.optimization_barrier((entries, level, *prepared))
    got = exchange(entries, PLANE)
    curvature, copies = bands(count, prepared, got, level)
    total_points = k_indices.shape[0] * count // 4
    total = jnp.sum(exchange(copies, ALL), axis=0) * (1.0 / math.sqrt(total_points))
    last = total[0:3, WF:].reshape(1, WF)
    totals = jnp.concatenate([total[:, :WF], last], axis=0)
    return (curvature.transpose(0, 2, 1), totals)


def solution(mesh):
    fine = Mesh(mesh.devices.reshape(4, 4, 2, 4), ALL)
    ka = ("z", "y", "core")
    in_specs = (P(ALL, None, None), P(ka, None, None, None), P(), P(ka, None), P(), P(), P())
    out_specs = (P(None, None, ALL), P())
    return jax.shard_map(
        on_device, mesh=fine, in_specs=in_specs, out_specs=out_specs, check_vma=False
    )
```
